512 devices in a mesh: dp: 16 (over y, x_lo), seq: 32 (over x_hi, z, core).
Axes of the slice: x: 4 (x_hi: 2, x_lo: 2; x = x_hi * 2 + x_lo), y: 8, z: 8, core: 2. Of those that a mesh axis runs over, the one named last changes fastest.
Arguments:
- queries: bfloat16 [16, 8192, 16, 128], P('dp', 'seq'), may hold values from -9 to 9
- keys: bfloat16 [16, 8192, 8, 128], P('dp', 'seq'), may hold values from -9 to 9
- values: bfloat16 [16, 8192, 8, 128], P('dp', 'seq'), may hold values from -6 to 6
- doc_lengths: int32 [16, 8], P('dp'), may hold values from 1 to 6144, 8192 in all within a row
Outputs:
- attended: bfloat16 [16, 8192, 16, 128], P('dp', 'seq')
- z_loss: float32 [], replicated
The draws below stay inside these ranges and needn't reach their ends.
Inputs may be any that keep to these rules, and one draw needn't show every extreme that they name: `doc_lengths`: each row's 8 lengths add up to 8192, and its longest document has exactly 6144 tokens.
All inputs are finite; a program needn't handle non-finite values.
Results may differ from the reference program's by a relative error of at most 0.012.
Values may be sent and summed in bfloat16 or wider, within the bound.
No kernel may reach another device: no remote copies, remote signals or barrier semaphores. Data moves between devices by JAX's collectives and lax.ppermute only.
A program may use at most 64 MiB of HBM per device.

```python
import math
import jax
import jax.numpy as jnp
import numpy as np
from jax import lax

HQ = 16
KVH = 8
HD = 128
WINDOW = 1024
DOCS = 8
TOK_DEV = 256
BATCH = 16
SEQ_LEN = 8192


def paired_vectors(key):
    query_shape = (BATCH, SEQ_LEN, HQ, HD)
    key_shape = (BATCH, SEQ_LEN, KVH, HD)
    query_draw = 1.5 * jnp.clip(jax.random.normal(jax.random.fold_in(key, 21), query_shape, jnp.float32), -6.0, 6.0)
    key_draw = 1.5 * jnp.clip(jax.random.normal(jax.random.fold_in(key, 22), key_shape, jnp.float32), -6.0, 6.0)
    return (query_draw, key_draw)


def draw_queries(key, part):
    return paired_vectors(key)[0].astype(jnp.bfloat16)


def draw_keys(key, part):
    return paired_vectors(key)[1].astype(jnp.bfloat16)


def steps_of(rng, dims, split, smallest, largest):
    factor_of, own = 1.0, jax.random.fold_in(rng, 6)
    for position, blocks in split:
        heights = jnp.exp(jax.random.uniform(jax.random.fold_in(own, position), (blocks,), jnp.float32, smallest / len(split), largest / len(split)))
        factor_of = factor_of * jnp.repeat(heights, dims[position] // blocks).reshape([-1 if axis == position else 1 for axis in range(len(dims))])
    return factor_of


def split_up(count, total, reach, lean):
    portions = [(1 << 20) // math.isqrt(rank ** lean) + 1 for rank in range(2, count + 1)]
    spare, given = total - reach - (count - 1), [1] * (count - 1)
    while spare > 0:
        candidates = [i for i in range(count - 1) if given[i] < reach]
        whole, left = sum([portions[i] for i in candidates]), spare
        for i in candidates:
            addition = min(reach - given[i], max(1, left * portions[i] // whole), spare)
            given[i] = given[i] + addition
            spare = spare - addition
    return np.array([reach] + given)


def ragged_sizes(rng, count, total, most, lean):
    if count == 2:
        one = jax.random.randint(rng, (), max(1, total - most), min(most, total - 1) + 1)
        return jnp.stack([one, total - one])
    lengths = jnp.asarray(split_up(count, total, most, lean), jnp.int32)
    pairs = (count - 1) // 2
    source_of, taker = lengths[1:1 + 2 * pairs:2], lengths[2:2 + 2 * pairs:2]
    slack = jnp.minimum(source_of - 1, most - taker)
    moved = jax.random.randint(jax.random.fold_in(rng, 1), (pairs,), 0, 1 << 20) % (slack + 1)
    lengths = lengths.at[1:1 + 2 * pairs:2].set(source_of - moved).at[2:2 + 2 * pairs:2].set(taker + moved)
    return lengths[jax.random.permutation(jax.random.fold_in(rng, 2), count)]


def gaussian(stream_key, extent, scale, most, cuts=(), kind=jnp.bfloat16):
    entries = jax.random.normal(stream_key, extent, jnp.float32) * scale
    if len(cuts) > 0:
        entries = steps_of(stream_key, extent, cuts, -0.22, 0.18) * entries
    return jnp.clip(entries, min=-most, max=most).astype(kind)


def setup_inputs(seed: int = 0) -> dict:
    arg_keys = jax.random.split(jax.random.key(seed), 5)
    return {
        "queries": draw_queries(jax.random.fold_in(arg_keys[4], 71), 0),
        "keys": draw_keys(jax.random.fold_in(arg_keys[4], 71), 0),
        "values": gaussian(arg_keys[2], (BATCH, SEQ_LEN, KVH, HD), 1.0, 6.0, ((0, 16), (1, 32))),
        "doc_lengths": jax.vmap(lambda own: ragged_sizes(own, DOCS, SEQ_LEN, 3 * SEQ_LEN // 4, 2))(jax.random.split(arg_keys[3], BATCH)).reshape((BATCH, DOCS)).astype(jnp.int32),
    }


rope_base = 500000.0
score_scale = 1.0 / 12.0
masked = -1.0e30


def rotate(tensor, places):
    half = tensor.shape[-1] // 2
    frequency = rope_base ** (-2.0 * jnp.arange(half, dtype=jnp.float32) / tensor.shape[-1])
    angles = places.astype(jnp.float32)[..., None, None] * frequency
    cos_table = jnp.cos(angles)
    sin_table = jnp.sin(angles)
    widened = tensor.astype(jnp.float32)
    front_half = widened[..., :half]
    back_half = widened[..., half:]
    joined = jnp.concatenate([front_half * cos_table - back_half * sin_table, back_half * cos_table + front_half * sin_table], axis=-1)
    return joined.astype(jnp.bfloat16)


def reference(queries, keys, values, doc_lengths):
    doc_ends = jnp.cumsum(doc_lengths, axis=1)
    doc_starts = doc_ends - doc_lengths
    all_rows = jnp.arange(SEQ_LEN, dtype=jnp.int32)
    doc_of = jnp.sum((doc_ends[:, None, :] <= all_rows[None, :, None]).astype(jnp.int32), axis=2)
    chosen = doc_of[:, :, None] == jnp.arange(DOCS, dtype=jnp.int32)[None, None, :]
    start_of = jnp.sum(jnp.where(chosen, doc_starts[:, None, :], 0), axis=2)
    places = all_rows[None, :] - start_of
    block = 512 if SEQ_LEN % 512 == 0 else TOK_DEV
    group_size = HQ // KVH

    def one_seq(operands):
        seq_queries, seq_keys, seq_values, seq_docs, seq_places = operands
        query_rot = rotate(seq_queries, seq_places)
        key_rot = rotate(seq_keys, seq_places)
        key_padded = jnp.pad(key_rot, ((WINDOW, 0), (0, 0), (0, 0)))
        value_padded = jnp.pad(seq_values, ((WINDOW, 0), (0, 0), (0, 0)))
        docs_padded = jnp.pad(seq_docs, (WINDOW, 0), constant_values=-1)

        def one_block(begin):
            query_block = lax.dynamic_slice_in_dim(query_rot, begin, block, 0).astype(jnp.float32)
            query_block = query_block.reshape(block, KVH, group_size, HD)
            key_block = lax.dynamic_slice_in_dim(key_padded, begin, WINDOW + block, 0).astype(jnp.float32)
            value_block = lax.dynamic_slice_in_dim(value_padded, begin, WINDOW + block, 0).astype(jnp.float32)
            query_docs = lax.dynamic_slice_in_dim(seq_docs, begin, block, 0)
            key_docs = lax.dynamic_slice_in_dim(docs_padded, begin, WINDOW + block, 0)
            query_at = begin + jnp.arange(block, dtype=jnp.int32)
            key_at = begin - WINDOW + jnp.arange(WINDOW + block, dtype=jnp.int32)
            visible = (query_docs[:, None] == key_docs[None, :]) & (key_at[None, :] <= query_at[:, None]) & (query_at[:, None] - key_at[None, :] < WINDOW)
            scores = jnp.einsum("tkgd,ukd->kgtu", query_block, key_block) * score_scale
            scores = jnp.where(visible[None, None], scores, masked)
            peak = jnp.max(scores, axis=-1)
            weights = jnp.where(visible[None, None], jnp.exp(scores - peak[..., None]), 0.0)
            total = jnp.sum(weights, axis=-1)
            rounded = weights.astype(jnp.bfloat16).astype(jnp.float32)
            mixed = jnp.einsum("kgtu,ukd->tkgd", rounded, value_block)
            mixed = mixed / jnp.transpose(total, (2, 0, 1))[..., None]
            return mixed.reshape(block, HQ, HD).astype(jnp.bfloat16), peak + jnp.log(total)

        begins = jnp.arange(SEQ_LEN // block, dtype=jnp.int32) * block
        outputs, normalizers = lax.map(one_block, begins)
        return outputs.reshape(SEQ_LEN, HQ, HD), jnp.sum(normalizers * normalizers)

    attended, squares = lax.map(one_seq, (queries, keys, values, doc_of, places))
    return attended, jnp.sum(squares) / (BATCH * SEQ_LEN * HQ)
```

```python
import functools
import math

import jax
import jax.numpy as jnp
from jax import lax
from jax.experimental import pallas as pl
from jax.experimental.pallas import tpu as pltpu
from jax.sharding import Mesh
from jax.sharding import PartitionSpec as P

WINDOW = 1024
SEQ = ("seq_0", "seq_1", "seq_2")
CHIP = ("seq_0", "seq_1")
DP_SEQ = ("dp_0", "dp_1", "seq_0", "seq_1", "seq_2")
DP = ("dp_0", "dp_1")
CORES = 2


rope_base = 500000.0
score_scale = 1.0 / 12.0
masked = -1e30
log2_e = 1.0 / math.log(2.0)
unit = score_scale * log2_e

VMEM = pl.BlockSpec(memory_space=pltpu.VMEM)
SMEM = pl.BlockSpec(memory_space=pltpu.SMEM)
NT = (((1,), (1,)), ((), ()))
TN = (((0,), (0,)), ((), ()))


def up_chip(block):
    count = lax.axis_size(SEQ)
    return lax.ppermute(block, SEQ, [(i, i + CORES) for i in range(count - CORES)])


def swapped(block):
    return lax.ppermute(block, "seq_2", [(0, 1), (1, 0)])


def rotated(block, cos_table, sin_table):
    wide = block.astype(jnp.float32)
    half = wide.shape[-1] // 2
    return (wide * cos_table + pltpu.roll(wide, half, 1) * sin_table).astype(jnp.bfloat16)


def doc_ends(lengths_ref):
    ends = [lengths_ref[0, 0]]
    for i in range(1, lengths_ref.shape[1]):
        ends.append(ends[-1] + lengths_ref[0, i])
    return ends


def doc_start(ends, at, low):
    for end in ends:
        low = jnp.maximum(low, jnp.where(at >= end, end, 0))
    return low


def block_start(spot_ref, rows, group, parity):
    core = spot_ref[1]
    place = core if parity == 0 else 1 - core
    return ((spot_ref[0] - group) * CORES + place) * rows


def single_slots(group, core):
    flip = core if group == 0 else 1 - core
    return [(0, 0, 0, None), (1, 1, 1, None), (0, 1, 2, flip == 1), (1, 0, 2, flip == 0)]


def guarded(condition, body):
    if condition is None:
        body()
    else:
        pl.when(condition)(body)


def table_kernel(lengths_ref, spot_ref, cos_ref, sin_ref):
    rows, width = cos_ref.shape[1:]
    half = width // 2
    pairs = rows // 2
    ends = doc_ends(lengths_ref)
    lane = lax.broadcasted_iota(jnp.int32, (pairs, width), 1)
    upper = lane >= half
    slot = jnp.where(upper, lane - half, lane).astype(jnp.float32)
    frequency = jnp.exp2(slot * (-2.0 * math.log2(rope_base) / width))
    sign = jnp.where(upper, 1.0, -1.0)
    for index in range(cos_ref.shape[0]):
        begin = block_start(spot_ref, rows, index // CORES, index % CORES)
        at = begin + lax.broadcasted_iota(jnp.int32, (pairs, width), 0)
        at = at + jnp.where(upper, pairs, 0)
        places = at - doc_start(ends, at, jnp.zeros_like(at))
        angles = places.astype(jnp.float32) * frequency
        for out_ref, table, factor in (
            (cos_ref, jnp.cos(angles), None),
            (sin_ref, jnp.sin(angles), sign),
        ):
            turned = pltpu.roll(table, half, 1)
            first = jnp.where(upper, turned, table)
            second = jnp.where(upper, table, turned)
            if factor is not None:
                first = first * factor
                second = second * factor
            out_ref[index, pl.ds(0, pairs), :] = first
            out_ref[index, pl.ds(pairs, pairs), :] = second


def bias_of(ends, spot_ref, rows, group, q_side, k_side):
    query_at = block_start(spot_ref, rows, 0, q_side) + lax.broadcasted_iota(
        jnp.int32, (1, rows), 1
    )
    key_at = block_start(spot_ref, rows, group, k_side) + lax.broadcasted_iota(
        jnp.int32, (rows, rows), 0
    )
    low = doc_start(ends, query_at, jnp.maximum(query_at - (WINDOW - 1), 0))
    bias = jnp.where((key_at >= low) & (key_at <= query_at), 0.0, masked)
    return jnp.concatenate([bias, bias], axis=1)


def gather_stats(
    group, lengths_ref, spot_ref, query_ref, key_of, weight_ref, mark_ref, peak_ref, total_ref
):
    heads = query_ref.shape[1]
    rows = weight_ref.shape[2]
    ends = doc_ends(lengths_ref)

    def visit(q_side, sides):
        biases = [bias_of(ends, spot_ref, rows, group, q_side, k_side) for k_side, _ in sides]
        for head in range(heads):
            row = pl.ds(q_side * heads + head, 1)
            old_peak = peak_ref[row, :]
            new_peak = old_peak
            parts = []
            for (k_side, _), bias in zip(sides, biases):
                scores = lax.dot_general(
                    key_of(k_side, head),
                    query_ref[q_side, head],
                    NT,
                    preferred_element_type=jnp.float32,
                )
                scores = scores + bias
                parts.append(scores)
                new_peak = jnp.maximum(new_peak, jnp.max(scores, axis=0, keepdims=True))
            total = total_ref[row, :] * jnp.exp2((old_peak - new_peak) * unit)
            for (_, slot), scores in zip(sides, parts):
                weights = jnp.exp2((scores - new_peak) * unit)
                total = total + jnp.sum(weights, axis=0, keepdims=True)
                weight_ref[slot, head] = weights.astype(jnp.bfloat16)
                mark_ref[slot, pl.ds(head, 1), :] = new_peak
            peak_ref[row, :] = new_peak
            total_ref[row, :] = total

    if group == 1:
        visit(0, [(0, 0), (1, 1)])
        visit(1, [(0, 2), (1, 3)])
        return
    for q_side, k_side, slot, condition in single_slots(group, spot_ref[1]):
        guarded(condition, functools.partial(visit, q_side, [(k_side, slot)]))


def rotate_keys(group, raw, cos_ref, sin_ref, key_ref):
    for side in range(CORES):
        cos_table = cos_ref[group * CORES + side]
        sin_table = sin_ref[group * CORES + side]
        for head in range(key_ref.shape[1]):
            key_ref[side, head] = rotated(raw(side, head), cos_table, sin_table)


def first_kernel(
    lengths_ref, spot_ref, cos_ref, sin_ref, k_own, k_other, q_own, q_other,
    query_ref, weight_ref, mark_ref, peak_ref, total_ref, key_ref,
):
    heads, rows = k_own.shape[:2]
    for side, raw_ref in enumerate((q_own, q_other)):
        cos_table = cos_ref[side]
        sin_table = sin_ref[side]
        for head in range(2 * heads):
            query_ref[side, head // 2, pl.ds((head % 2) * rows, rows), :] = rotated(
                raw_ref[head], cos_table, sin_table
            )
    raw = (k_own, k_other)
    rotate_keys(0, lambda side, head: raw[side][head], cos_ref, sin_ref, key_ref)
    peak_ref[...] = jnp.full_like(peak_ref, masked)
    total_ref[...] = jnp.zeros_like(total_ref)
    gather_stats(
        0, lengths_ref, spot_ref, query_ref, lambda s, h: key_ref[s, h],
        weight_ref, mark_ref, peak_ref, total_ref,
    )


def next_kernel(
    lengths_ref, spot_ref, cos_ref, sin_ref, k_own, k_other, query_ref, old_peak, old_total,
    weight_ref, mark_ref, peak_ref, total_ref, key_ref,
):
    raw = (k_own, k_other)
    rotate_keys(1, lambda side, head: raw[side][head], cos_ref, sin_ref, key_ref)
    peak_ref[...] = old_peak[...]
    total_ref[...] = old_total[...]
    gather_stats(
        1, lengths_ref, spot_ref, query_ref, lambda s, h: key_ref[s, h],
        weight_ref, mark_ref, peak_ref, total_ref,
    )


def last_kernel(
    lengths_ref, spot_ref, cos_ref, sin_ref, k_own, k_other, query_ref, old_peak, old_total,
    weight_ref, mark_ref, level_ref, squares_ref, peak_ref, total_ref, key_ref,
):
    raw = (k_own, k_other)
    rotate_keys(2, lambda side, head: raw[side][head], cos_ref, sin_ref, key_ref)
    peak_ref[...] = old_peak[...]
    total_ref[...] = old_total[...]
    gather_stats(
        2, lengths_ref, spot_ref, query_ref, lambda s, h: key_ref[s, h],
        weight_ref, mark_ref, peak_ref, total_ref,
    )
    natural = peak_ref[...] * score_scale + jnp.log(total_ref[...])
    level_ref[...] = natural * log2_e
    squares = jnp.sum(natural * natural, axis=(0, 1), keepdims=True)
    squares_ref[...] = jnp.broadcast_to(squares, squares_ref.shape)


def weighed(weight_ref, mark_ref, level_ref, value, q_side, head, heads, slot):
    scale = jnp.exp2(
        mark_ref[slot, pl.ds(head, 1), :] * unit - level_ref[pl.ds(q_side * heads + head, 1), :]
    )
    return scale * lax.dot_general(
        value, weight_ref[slot, head], TN, preferred_element_type=jnp.float32
    )


def near_kernel(
    spot_ref, level_ref, weight_0, mark_0, weight_1, mark_1, v0_own, v0_other, v1_ref, sum_ref
):
    heads = v0_own.shape[0]
    v0 = (v0_own, v0_other)
    for q_side in range(CORES):
        for head in range(heads):
            part = functools.partial(weighed, q_side=q_side, head=head, heads=heads)
            far = v1_ref[head], v1_ref[heads + head]
            sum_ref[q_side, head] = (
                part(weight_0, mark_0, level_ref, v0[q_side][head], slot=q_side)
                + part(weight_1, mark_1, level_ref, far[0], slot=2 * q_side)
                + part(weight_1, mark_1, level_ref, far[1], slot=2 * q_side + 1)
            )

    def cross(q_side, k_side, slot):
        for head in range(heads):
            sum_ref[q_side, head] += weighed(
                weight_0, mark_0, level_ref, v0[k_side][head], q_side, head, heads, slot
            )

    for q_side, k_side, slot, condition in single_slots(0, spot_ref[1])[2:]:
        guarded(condition, functools.partial(cross, q_side, k_side, slot))


def far_kernel(spot_ref, level_ref, weight_2, mark_2, v2_ref, near_ref, own_ref, other_ref, sum_ref):
    heads = near_ref.shape[1]
    for q_side in range(CORES):
        for head in range(heads):
            sum_ref[q_side, head] = near_ref[q_side, head] + weighed(
                weight_2, mark_2, level_ref, v2_ref[q_side * heads + head],
                q_side, head, heads, q_side,
            )

    def cross(q_side, k_side, slot):
        for head in range(heads):
            sum_ref[q_side, head] += weighed(
                weight_2, mark_2, level_ref, v2_ref[k_side * heads + head],
                q_side, head, heads, slot,
            )

    for q_side, k_side, slot, condition in single_slots(2, spot_ref[1])[2:]:
        guarded(condition, functools.partial(cross, q_side, k_side, slot))
    rows = own_ref.shape[1]
    for side, out_ref in enumerate((own_ref, other_ref)):
        for head in range(heads):
            for member in range(2):
                block = sum_ref[side, head, :, pl.ds(member * rows, rows)]
                out_ref[head * 2 + member] = jnp.transpose(block, (1, 0)).astype(jnp.bfloat16)


def call(kernel, out_shape, scalars, count, flops, scratch=()):
    def run(*operands):
        return pl.pallas_call(
            kernel,
            out_shape=out_shape,
            in_specs=[SMEM] * scalars + [VMEM] * (count - scalars),
            out_specs=jax.tree.map(lambda _: VMEM, out_shape),
            scratch_shapes=list(scratch),
            cost_estimate=pl.CostEstimate(flops=flops, bytes_accessed=0, transcendentals=0),
        )(*operands)

    return run


def halves(tensor, core):
    by_head = jnp.transpose(tensor, (1, 0, 2))
    part = by_head.shape[0] // CORES
    mine = lax.dynamic_slice_in_dim(by_head, core * part, part, 0)
    give = lax.dynamic_slice_in_dim(by_head, (1 - core) * part, part, 0)
    return mine, give


def after(value, *others):
    return lax.optimization_barrier((value, *others))[0]


def device_part(queries, keys, values, doc_lengths):
    rows, query_heads, width = queries.shape[1:]
    key_heads = keys.shape[2]
    heads = key_heads // CORES
    members = query_heads // key_heads
    devices = lax.axis_size(DP_SEQ)
    core = lax.axis_index("seq_2")
    chip = lax.axis_index(CHIP)
    f32, bf16 = jnp.float32, jnp.bfloat16
    shape = jax.ShapeDtypeStruct
    spot = jnp.stack([chip, core]).astype(jnp.int32)

    k_mine, k_give = halves(keys[0], core)
    k1_own = up_chip(k_mine)
    k0_other = swapped(k_give)
    k1_other = up_chip(k0_other)
    k2_own = up_chip(k1_own)
    q_mine, q_give = halves(queries[0], core)
    v_mine, v_give = halves(values[0], core)
    give = jnp.concatenate([q_give, v_give], axis=0)
    got = swapped(give)
    q_other, v0_other = got[: heads * members], got[heads * members :]

    table = shape((3 * CORES, rows, width), f32)
    cos_table, sin_table = call(table_kernel, (table, table), 2, 2, TABLE_FLOPS)(doc_lengths, spot)
    k2_other = up_chip(k1_other)
    v1 = up_chip(jnp.concatenate([v_mine, v0_other], axis=0))

    stats = shape((CORES * heads, members * rows), f32)
    q_shape = shape((CORES, heads, members * rows, width), bf16)
    key_scratch = pltpu.VMEM((CORES, heads, rows, width), bf16)

    def slots(count):
        return (
            shape((count, heads, rows, members * rows), bf16),
            shape((count, heads, members * rows), f32),
        )

    query_rot, weight_0, mark_0, peak, total = call(
        first_kernel, (q_shape, *slots(3), stats, stats), 2, 8, FIRST_FLOPS, (key_scratch,)
    )(doc_lengths, spot, cos_table, sin_table, k_mine, k0_other, q_mine, q_other)
    weight_1, mark_1, peak, total = call(
        next_kernel, (*slots(4), stats, stats), 2, 9, NEXT_FLOPS, (key_scratch,)
    )(doc_lengths, spot, cos_table, sin_table, k1_own, k1_other, query_rot, peak, total)
    weight_2, mark_2, level, squares = call(
        last_kernel,
        (*slots(3), stats, shape((16, width), f32)),
        2,
        9,
        NEXT_FLOPS,
        (pltpu.VMEM(stats.shape, f32), pltpu.VMEM(stats.shape, f32), key_scratch),
    )(doc_lengths, spot, cos_table, sin_table, k2_own, k2_other, query_rot, peak, total)
    squares = sum_over(("seq_1", "seq_2"), squares)
    v2 = up_chip(after(v1, squares))
    squares = sum_over(("dp_0", "dp_1", "seq_0"), squares)
    z_loss = squares[0, 0] / (devices * rows * query_heads)

    sum_shape = shape((CORES, heads, width, members * rows), f32)
    near = call(near_kernel, sum_shape, 1, 9, NEAR_FLOPS)(
        spot, level, weight_0, mark_0, weight_1, mark_1, v_mine, v0_other, v1
    )
    out_shape = shape((heads * members, rows, width), bf16)
    own, other = call(
        far_kernel, (out_shape, out_shape), 1, 6, NEAR_FLOPS,
        (pltpu.VMEM(sum_shape.shape, f32),),
    )(spot, level, weight_2, mark_2, v2, near)
    partner = swapped(other)
    low = jnp.where(core == 0, own, partner)
    high = jnp.where(core == 0, partner, own)
    attended = jnp.transpose(jnp.concatenate([low, high], axis=0), (1, 0, 2))
    return (attended[None], z_loss)


def sum_over(axes, part):
    count = lax.axis_size(axes)
    spread = jnp.broadcast_to(part[:1], (count, part.shape[1]))
    return jnp.sum(lax.all_to_all(spread, axes, 0, 0), axis=0, keepdims=True)


TABLE_FLOPS = 4_000_000
FIRST_FLOPS = 6_000_000
NEXT_FLOPS = 6_000_000
NEAR_FLOPS = 3_000_000


def solution(mesh):
    torus = Mesh(mesh.devices.reshape(8, 2, 2, 8, 2), ("dp_0", "dp_1", "seq_0", "seq_1", "seq_2"))
    in_specs = (P(DP, SEQ, None, None), P(DP, SEQ, None, None), P(DP, SEQ, None, None), P(DP, None))
    out_specs = (P(DP, SEQ, None, None), P())
    return jax.shard_map(
        device_part, mesh=torus, in_specs=in_specs, out_specs=out_specs, check_vma=False
    )
```

```python
import functools
import math

import jax
import jax.numpy as jnp
from jax import lax
from jax.experimental import pallas as pl
from jax.experimental.pallas import tpu as pltpu
from jax.sharding import Mesh
from jax.sharding import PartitionSpec as P

WINDOW = 1024
SEQ = ("seq_0", "seq_1", "seq_2")
CHIP = ("seq_0", "seq_1")
DP_SEQ = ("dp_0", "dp_1", "seq_0", "seq_1", "seq_2")
DP = ("dp_0", "dp_1")
CORES = 2


rope_base = 500000.0
score_scale = 1.0 / 12.0
masked = -1e30
log2_e = 1.0 / math.log(2.0)
unit = score_scale * log2_e

VMEM = pl.BlockSpec(memory_space=pltpu.VMEM)
SMEM = pl.BlockSpec(memory_space=pltpu.SMEM)
HBM = pl.BlockSpec(memory_space=pltpu.HBM)
NT = (((1,), (1,)), ((), ()))
TN = (((0,), (0,)), ((), ()))


def up_chip(block, chips=1):
    count = lax.axis_size(SEQ)
    step = chips * CORES
    return lax.ppermute(block, SEQ, [(i, i + step) for i in range(count - step)])


def swapped(block):
    return lax.ppermute(block, "seq_2", [(0, 1), (1, 0)])


def rotated(block, cos_table, sin_table):
    wide = block.astype(jnp.float32)
    half = wide.shape[-1] // 2
    return (wide * cos_table + pltpu.roll(wide, half, 1) * sin_table).astype(jnp.bfloat16)


def doc_ends(lengths_ref):
    ends = [lengths_ref[0, 0]]
    for i in range(1, lengths_ref.shape[1]):
        ends.append(ends[-1] + lengths_ref[0, i])
    return ends


def doc_start(ends, at, low):
    for end in ends:
        low = jnp.maximum(low, jnp.where(at >= end, end, 0))
    return low


def block_start(spot_ref, rows, group, parity):
    core = spot_ref[1]
    place = core if parity == 0 else 1 - core
    return ((spot_ref[0] - group) * CORES + place) * rows


def single_slots(group, core):
    flip = core if group == 0 else 1 - core
    return [(0, 0, 0, None), (1, 1, 1, None), (0, 1, 2, flip == 1), (1, 0, 2, flip == 0)]


def guarded(condition, body):
    if condition is None:
        body()
    else:
        pl.when(condition)(body)


def table_kernel(lengths_ref, spot_ref, cos_ref, sin_ref):
    rows, width = cos_ref.shape[1:]
    half = width // 2
    pairs = rows // 2
    ends = doc_ends(lengths_ref)
    lane = lax.broadcasted_iota(jnp.int32, (pairs, width), 1)
    upper = lane >= half
    slot = jnp.where(upper, lane - half, lane).astype(jnp.float32)
    frequency = jnp.exp2(slot * (-2.0 * math.log2(rope_base) / width))
    sign = jnp.where(upper, 1.0, -1.0)
    for index in range(cos_ref.shape[0]):
        begin = block_start(spot_ref, rows, index // CORES, index % CORES)
        at = begin + lax.broadcasted_iota(jnp.int32, (pairs, width), 0)
        at = at + jnp.where(upper, pairs, 0)
        places = at - doc_start(ends, at, jnp.zeros_like(at))
        angles = places.astype(jnp.float32) * frequency
        for out_ref, table, factor in (
            (cos_ref, jnp.cos(angles), None),
            (sin_ref, jnp.sin(angles), sign),
        ):
            turned = pltpu.roll(table, half, 1)
            first = jnp.where(upper, turned, table)
            second = jnp.where(upper, table, turned)
            if factor is not None:
                first = first * factor
                second = second * factor
            out_ref[index, pl.ds(0, pairs), :] = first
            out_ref[index, pl.ds(pairs, pairs), :] = second


def bias_of(ends, spot_ref, rows, group, q_side, k_side):
    query_at = block_start(spot_ref, rows, 0, q_side) + lax.broadcasted_iota(
        jnp.int32, (1, rows), 1
    )
    key_at = block_start(spot_ref, rows, group, k_side) + lax.broadcasted_iota(
        jnp.int32, (rows, rows), 0
    )
    low = doc_start(ends, query_at, jnp.maximum(query_at - (WINDOW - 1), 0))
    bias = jnp.where((key_at >= low) & (key_at <= query_at), 0.0, masked)
    return jnp.concatenate([bias, bias], axis=1)


def gather_stats(
    group, lengths_ref, spot_ref, query_ref, key_of, weight_ref, mark_ref, peak_ref, total_ref,
    stage_ref, sent,
):
    heads = query_ref.shape[1]
    rows = weight_ref.shape[2]
    ends = doc_ends(lengths_ref)

    def copy_out(slot, head):
        return pltpu.make_async_copy(
            stage_ref.at[slot, head], weight_ref.at[slot, head], sent.at[slot, head]
        )

    def visit(q_side, sides):
        biases = [bias_of(ends, spot_ref, rows, group, q_side, k_side) for k_side, _ in sides]

        def scored(head):
            return [
                lax.dot_general(
                    key_of(k_side, head),
                    query_ref[q_side, head],
                    NT,
                    preferred_element_type=jnp.float32,
                )
                + bias
                for (k_side, _), bias in zip(sides, biases)
            ]

        for head in range(heads):
            parts = scored(head)
            row = pl.ds(q_side * heads + head, 1)
            old_peak = peak_ref[row, :]
            new_peak = old_peak
            for scores in parts:
                new_peak = jnp.maximum(new_peak, jnp.max(scores, axis=0, keepdims=True))
            total = total_ref[row, :] * jnp.exp2((old_peak - new_peak) * unit)
            for (_, slot), scores in zip(sides, parts):
                weights = jnp.exp2((scores - new_peak) * unit)
                total = total + jnp.sum(weights, axis=0, keepdims=True)
                stage_ref[slot, head] = weights.astype(jnp.bfloat16)
                mark_ref[slot, pl.ds(head, 1), :] = new_peak
            peak_ref[row, :] = new_peak
            total_ref[row, :] = total
            for _, slot in sides:
                copy_out(slot, head).start()

    if group == 1:
        visit(0, [(0, 0), (1, 1)])
        visit(1, [(0, 2), (1, 3)])
    else:
        for q_side, k_side, slot, condition in single_slots(group, spot_ref[1]):
            guarded(condition, functools.partial(visit, q_side, [(k_side, slot)]))

    def wait_all():
        for slot in range(weight_ref.shape[0]):
            for head in range(heads):
                copy_out(slot, head).wait()

    return wait_all


def rotate_keys(group, raw, cos_ref, sin_ref, key_ref):
    for side in range(CORES):
        cos_table = cos_ref[group * CORES + side]
        sin_table = sin_ref[group * CORES + side]
        for head in range(key_ref.shape[1]):
            key_ref[side, head] = rotated(raw(side, head), cos_table, sin_table)


def first_kernel(
    lengths_ref, spot_ref, cos_ref, sin_ref, k_all, k_other, q_all, v_all, got_ref,
    query_ref, value_ref, weight_ref, mark_ref, peak_ref, total_ref, key_ref, stage_ref, sent,
):
    heads, rows = k_other.shape[:2]
    core = spot_ref[1]
    for side in range(CORES):
        cos_table = cos_ref[side]
        sin_table = sin_ref[side]
        for head in range(2 * heads):
            raw = q_all[core * 2 * heads + head] if side == 0 else got_ref[head]
            query_ref[side, head // 2, pl.ds((head % 2) * rows, rows), :] = rotated(
                raw, cos_table, sin_table
            )

    def raw_key(side, head):
        return k_all[core * heads + head] if side == 0 else k_other[head]

    for head in range(heads):
        value_ref[head] = v_all[core * heads + head]
        value_ref[heads + head] = got_ref[2 * heads + head]
    rotate_keys(0, raw_key, cos_ref, sin_ref, key_ref)
    peak_ref[...] = jnp.full_like(peak_ref, masked)
    total_ref[...] = jnp.zeros_like(total_ref)
    gather_stats(
        0, lengths_ref, spot_ref, query_ref, lambda s, h: key_ref[s, h],
        weight_ref, mark_ref, peak_ref, total_ref, stage_ref, sent,
    )()


def rest_kernel(
    lengths_ref, spot_ref, cos_ref, sin_ref, k1_own, k1_other, k2_own, k2_other, query_ref,
    old_peak, old_total,
    weight_1, mark_1, weight_2, mark_2, level_ref, squares_ref,
    peak_ref, total_ref, key_1, stage_1, sent_1, key_2, stage_2, sent_2,
):
    peak_ref[...] = old_peak[...]
    total_ref[...] = old_total[...]
    waits = []
    for group, raw, key_ref, weight_ref, mark_ref, stage_ref, sent in (
        (1, (k1_own, k1_other), key_1, weight_1, mark_1, stage_1, sent_1),
        (2, (k2_own, k2_other), key_2, weight_2, mark_2, stage_2, sent_2),
    ):
        rotate_keys(group, lambda side, head: raw[side][head], cos_ref, sin_ref, key_ref)
        waits.append(
            gather_stats(
                group, lengths_ref, spot_ref, query_ref, lambda s, h: key_ref[s, h],
                weight_ref, mark_ref, peak_ref, total_ref, stage_ref, sent,
            )
        )
    natural = peak_ref[...] * score_scale + jnp.log(total_ref[...])
    level_ref[...] = natural * log2_e
    squares = jnp.sum(natural * natural, axis=(0, 1), keepdims=True)
    squares_ref[...] = jnp.broadcast_to(squares, squares_ref.shape)
    for wait_all in waits:
        wait_all()


def fetch(weight_ref, held_ref, ready):
    def copy(slot):
        return pltpu.make_async_copy(weight_ref.at[slot], held_ref.at[slot], ready.at[slot, 0])

    return copy


def weighed(weight_ref, mark_ref, level_ref, value, q_side, head, heads, slot):
    scale = jnp.exp2(
        mark_ref[slot, pl.ds(head, 1), :] * unit - level_ref[pl.ds(q_side * heads + head, 1), :]
    )
    return scale * lax.dot_general(
        value, weight_ref[slot, head], TN, preferred_element_type=jnp.float32
    )


def near_kernel(
    spot_ref, level_ref, weight_0, mark_0, weight_1, mark_1, v0_ref, v1_ref, sum_ref,
    held_0, held_1, ready_0, ready_1,
):
    heads = sum_ref.shape[1]
    copies_0 = fetch(weight_0, held_0, ready_0)
    copies_1 = fetch(weight_1, held_1, ready_1)
    for copy in (
        copies_0(0), copies_1(0), copies_1(1), copies_0(1), copies_1(2), copies_1(3), copies_0(2)
    ):
        copy.start()
    for q_side in range(CORES):
        for copy in (copies_0(q_side), copies_1(2 * q_side), copies_1(2 * q_side + 1)):
            copy.wait()
        for head in range(heads):
            part = functools.partial(weighed, q_side=q_side, head=head, heads=heads)
            sum_ref[q_side, head] = (
                part(held_0, mark_0, level_ref, v0_ref[q_side * heads + head], slot=q_side)
                + part(held_1, mark_1, level_ref, v1_ref[head], slot=2 * q_side)
                + part(held_1, mark_1, level_ref, v1_ref[heads + head], slot=2 * q_side + 1)
            )
    copies_0(2).wait()

    def cross(q_side, k_side, slot):
        for head in range(heads):
            sum_ref[q_side, head] += weighed(
                held_0, mark_0, level_ref, v0_ref[k_side * heads + head], q_side, head, heads, slot
            )

    for q_side, k_side, slot, condition in single_slots(0, spot_ref[1])[2:]:
        guarded(condition, functools.partial(cross, q_side, k_side, slot))


def far_kernel(
    side, spot_ref, level_ref, weight_2, mark_2, v2_ref, near_ref, out_ref,
    sum_ref, held, ready,
):
    heads = near_ref.shape[1]
    copies = fetch(weight_2, held, ready)
    cross_here = [entry for entry in single_slots(2, spot_ref[1])[2:] if entry[0] == side]
    for slot in (2, side):
        copies(slot).start()
    sum_ref[...] = near_ref[side]
    copies(2).wait()

    def cross(k_side, slot):
        for head in range(heads):
            sum_ref[head] += weighed(
                held, mark_2, level_ref, v2_ref[k_side * heads + head], side, head, heads, slot
            )

    for _, k_side, slot, condition in cross_here:
        guarded(condition, functools.partial(cross, k_side, slot))
    rows = out_ref.shape[1]
    copies(side).wait()
    for head in range(heads):
        block = sum_ref[head] + weighed(
            held, mark_2, level_ref, v2_ref[side * heads + head], side, head, heads, side
        )
        turned = jnp.transpose(block, (1, 0)).astype(jnp.bfloat16)
        out_ref[head * 2] = turned[:rows]
        out_ref[head * 2 + 1] = turned[rows:]


def call(kernel, out_shape, scalars, count, flops, scratch=(), far_in=(), far_out=()):
    def run(*operands):
        return pl.pallas_call(
            kernel,
            out_shape=out_shape,
            in_specs=[SMEM] * scalars
            + [HBM if i in far_in else VMEM for i in range(scalars, count)],
            out_specs=tuple(
                HBM if i in far_out else VMEM for i in range(len(out_shape))
            ),
            scratch_shapes=list(scratch),
            cost_estimate=pl.CostEstimate(flops=flops, bytes_accessed=0, transcendentals=0),
            compiler_params=pltpu.CompilerParams(vmem_limit_bytes=VMEM_LIMIT),
        )(*operands)

    return run


def by_head(tensor):
    return lax.optimization_barrier(jnp.transpose(tensor, (1, 0, 2)))


def half_of(tensor, core):
    part = tensor.shape[0] // CORES
    return jnp.where(core == 0, tensor[:part], tensor[part:])


def device_part(queries, keys, values, doc_lengths):
    rows, query_heads, width = queries.shape[1:]
    key_heads = keys.shape[2]
    heads = key_heads // CORES
    members = query_heads // key_heads
    devices = lax.axis_size(DP_SEQ)
    core = lax.axis_index("seq_2")
    chip = lax.axis_index(CHIP)
    f32, bf16 = jnp.float32, jnp.bfloat16
    shape = jax.ShapeDtypeStruct
    spot = jnp.stack([chip, core]).astype(jnp.int32)

    k_all = by_head(keys[0])
    k1_own = up_chip(half_of(k_all, core))
    k0_other = swapped(half_of(k_all, 1 - core))
    k1_other = up_chip(k0_other)
    k2_own = up_chip(k1_own)
    q_all = by_head(queries[0])
    v_all = by_head(values[0])
    give = jnp.concatenate([half_of(q_all, 1 - core), half_of(v_all, 1 - core)], axis=0)
    got = swapped(give)

    table = shape((3 * CORES, rows, width), f32)
    cos_table, sin_table = call(table_kernel, (table, table), 2, 2, TABLE_FLOPS)(doc_lengths, spot)
    k2_other = up_chip(k1_other)

    stats = shape((CORES * heads, members * rows), f32)
    q_shape = shape((CORES, heads, members * rows, width), bf16)
    key_scratch = pltpu.VMEM((CORES, heads, rows, width), bf16)

    def slots(count):
        return (
            pltpu.HBM((count, heads, rows, members * rows), bf16),
            shape((count, heads, members * rows), f32),
        )

    def staged(count):
        return (
            key_scratch,
            pltpu.VMEM((count, heads, rows, members * rows), bf16),
            pltpu.SemaphoreType.DMA((count, heads)),
        )

    v_shape = shape((CORES * heads, rows, width), bf16)
    query_rot, v0, weight_0, mark_0, peak, total = call(
        first_kernel, (q_shape, v_shape, *slots(3), stats, stats), 2, 9, FIRST_FLOPS,
        staged(3), far_out=(2,),
    )(doc_lengths, spot, cos_table, sin_table, k_all, k0_other, q_all, v_all, got)
    v1 = up_chip(v0)
    v2 = up_chip(v1)
    weight_1, mark_1, weight_2, mark_2, level, squares = call(
        rest_kernel,
        (*slots(4), *slots(3), stats, shape((16, width), f32)),
        2,
        11,
        NEXT_FLOPS,
        (
            pltpu.VMEM(stats.shape, f32), pltpu.VMEM(stats.shape, f32),
            *staged(4), *staged(3),
        ),
        far_out=(0, 2),
    )(
        doc_lengths, spot, cos_table, sin_table, k1_own, k1_other, k2_own, k2_other, query_rot,
        peak, total,
    )
    squares = sum_over(("seq_1", "seq_2"), squares)
    squares = sum_over(("dp_0", "dp_1", "seq_0"), squares)
    z_loss = squares[0, 0] / (devices * rows * query_heads)

    weight_0, weight_1, weight_2 = (
        pltpu.with_memory_space_constraint(array, pltpu.HBM)
        for array in (weight_0, weight_1, weight_2)
    )
    sum_shape = shape((CORES, heads, width, members * rows), f32)
    (near,) = call(
        near_kernel, (sum_shape,), 1, 8, NEAR_FLOPS,
        (*staged(3)[1:2], *staged(4)[1:2], *staged(3)[2:], *staged(4)[2:]),
        far_in=(2, 4),
    )(spot, level, weight_0, mark_0, weight_1, mark_1, v0, v1)
    out_shape = shape((heads * members, rows, width), bf16)
    own, other = (
        call(
            functools.partial(far_kernel, side), (out_shape,), 1, 6, NEAR_FLOPS,
            (pltpu.VMEM(sum_shape.shape[1:], f32), *staged(3)[1:]),
            far_in=(2,),
        )(spot, level, weight_2, mark_2, v2, near)[0]
        for side in range(2)
    )
    partner = swapped(other)
    low = jnp.where(core == 0, own, partner)
    high = jnp.where(core == 0, partner, own)
    attended = jnp.transpose(jnp.concatenate([low, high], axis=0), (1, 0, 2))
    return (attended[None], z_loss)


def sum_over(axes, part):
    count = lax.axis_size(axes)
    spread = jnp.broadcast_to(part[:1], (count, part.shape[1]))
    return jnp.sum(lax.all_to_all(spread, axes, 0, 0), axis=0, keepdims=True)


VMEM_LIMIT = 20 * 1024 * 1024
TABLE_FLOPS = 4_000_000
FIRST_FLOPS = 6_000_000
NEXT_FLOPS = 6_000_000
NEAR_FLOPS = 3_000_000


def solution(mesh):
    torus = Mesh(mesh.devices.reshape(8, 2, 2, 8, 2), ("dp_0", "dp_1", "seq_0", "seq_1", "seq_2"))
    in_specs = (P(DP, SEQ, None, None), P(DP, SEQ, None, None), P(DP, SEQ, None, None), P(DP, None))
    out_specs = (P(DP, SEQ, None, None), P())
    return jax.shard_map(
        device_part, mesh=torus, in_specs=in_specs, out_specs=out_specs, check_vma=False
    )
```

```python
import functools
import math

import jax
import jax.numpy as jnp
from jax import lax
from jax.experimental import pallas as pl
from jax.experimental.pallas import tpu as pltpu
from jax.sharding import Mesh
from jax.sharding import PartitionSpec as P

WINDOW = 1024
SEQ = ("seq_0", "seq_1", "seq_2")
CHIP = ("seq_0", "seq_1")
DP_SEQ = ("dp_0", "dp_1", "seq_0", "seq_1", "seq_2")
DP = ("dp_0", "dp_1")
CORES = 2


rope_base = 500000.0
score_scale = 1.0 / 12.0
masked = -1e30
log2_e = 1.0 / math.log(2.0)
unit = score_scale * log2_e

VMEM = pl.BlockSpec(memory_space=pltpu.VMEM)
SMEM = pl.BlockSpec(memory_space=pltpu.SMEM)
HBM = pl.BlockSpec(memory_space=pltpu.HBM)
NT = (((1,), (1,)), ((), ()))
TN = (((0,), (0,)), ((), ()))


def up_chip(block, chips=1):
    count = lax.axis_size(SEQ)
    step = chips * CORES
    return lax.ppermute(block, SEQ, [(i, i + step) for i in range(count - step)])


def swapped(block):
    return lax.ppermute(block, "seq_2", [(0, 1), (1, 0)])


def rotated(block, cos_table, sin_table):
    wide = block.astype(jnp.float32)
    half = wide.shape[-1] // 2
    return (wide * cos_table + pltpu.roll(wide, half, 1) * sin_table).astype(jnp.bfloat16)


def doc_ends(lengths_ref):
    ends = [lengths_ref[0, 0]]
    for i in range(1, lengths_ref.shape[1]):
        ends.append(ends[-1] + lengths_ref[0, i])
    return ends


def doc_start(ends, at, low):
    for end in ends:
        low = jnp.maximum(low, jnp.where(at >= end, end, 0))
    return low


def block_start(spot_ref, rows, group, parity):
    core = spot_ref[1]
    place = core if parity == 0 else 1 - core
    return ((spot_ref[0] - group) * CORES + place) * rows


def single_slots(group, core):
    flip = core if group == 0 else 1 - core
    return [(0, 0, 0, None), (1, 1, 1, None), (0, 1, 2, flip == 1), (1, 0, 2, flip == 0)]


def guarded(condition, body):
    if condition is None:
        body()
    else:
        pl.when(condition)(body)


def cos_sin(angles):
    turns = jnp.floor(angles * (2.0 / math.pi) + 0.5)
    rest = ((angles - turns * 1.5703125) - turns * 4.837512969970703125e-4) - turns * 7.54978995489188216e-8
    square = rest * rest
    sine = (
        (-1.9515295891e-4 * square + 8.3321608736e-3) * square - 1.6666654611e-1
    ) * square * rest + rest
    cosine = (
        (2.443315711809948e-5 * square - 1.388731625493765e-3) * square + 4.166664568298827e-2
    ) * square * square - 0.5 * square + 1.0
    quarter = turns.astype(jnp.int32)
    odd = (quarter & 1) == 1
    return (
        jnp.where(((quarter + 1) & 2) == 2, -1.0, 1.0) * jnp.where(odd, sine, cosine),
        jnp.where((quarter & 2) == 2, -1.0, 1.0) * jnp.where(odd, cosine, sine),
    )


def table_kernel(lengths_ref, spot_ref, frequency_ref, cos_ref, sin_ref):
    rows, width = cos_ref.shape[1:]
    half = width // 2
    pairs = rows // 2
    ends = doc_ends(lengths_ref)
    upper = lax.broadcasted_iota(jnp.int32, (pairs, width), 1) >= half
    sign = jnp.where(upper, 1.0, -1.0)
    frequency = frequency_ref[...]
    for index in range(cos_ref.shape[0]):
        begin = block_start(spot_ref, rows, index // CORES, index % CORES)
        at = begin + lax.broadcasted_iota(jnp.int32, (pairs, width), 0)
        at = at + jnp.where(upper, pairs, 0)
        places = at - doc_start(ends, at, jnp.zeros_like(at))
        cosine, sine = cos_sin(places.astype(jnp.float32) * frequency)
        for out_ref, table, factor in ((cos_ref, cosine, None), (sin_ref, sine, sign)):
            turned = pltpu.roll(table, half, 1)
            first = jnp.where(upper, turned, table)
            second = jnp.where(upper, table, turned)
            if factor is not None:
                first = first * factor
                second = second * factor
            out_ref[index, pl.ds(0, pairs), :] = first
            out_ref[index, pl.ds(pairs, pairs), :] = second


def bias_of(ends, spot_ref, rows, group, q_side, k_side):
    query_at = block_start(spot_ref, rows, 0, q_side) + lax.broadcasted_iota(
        jnp.int32, (1, rows), 1
    )
    key_at = block_start(spot_ref, rows, group, k_side) + lax.broadcasted_iota(
        jnp.int32, (rows, rows), 0
    )
    low = doc_start(ends, query_at, jnp.maximum(query_at - (WINDOW - 1), 0))
    bias = jnp.where((key_at >= low) & (key_at <= query_at), 0.0, masked)
    return jnp.concatenate([bias, bias], axis=1)


def gather_stats(
    group, lengths_ref, spot_ref, query_ref, key_of, weight_ref, mark_ref, peak_ref, total_ref,
    stage_ref, sent,
):
    heads = query_ref.shape[1]
    rows = weight_ref.shape[2]
    ends = doc_ends(lengths_ref)

    def copy_out(slot, head):
        return pltpu.make_async_copy(
            stage_ref.at[slot, head], weight_ref.at[slot, head], sent.at[slot, head]
        )

    def visit(q_side, sides):
        biases = [bias_of(ends, spot_ref, rows, group, q_side, k_side) for k_side, _ in sides]

        def scored(head):
            return [
                lax.dot_general(
                    key_of(k_side, head),
                    query_ref[q_side, head],
                    NT,
                    preferred_element_type=jnp.float32,
                )
                + bias
                for (k_side, _), bias in zip(sides, biases)
            ]

        for head in range(heads):
            parts = scored(head)
            row = pl.ds(q_side * heads + head, 1)
            old_peak = peak_ref[row, :]
            new_peak = old_peak
            for scores in parts:
                new_peak = jnp.maximum(new_peak, jnp.max(scores, axis=0, keepdims=True))
            total = total_ref[row, :] * jnp.exp2((old_peak - new_peak) * unit)
            for (_, slot), scores in zip(sides, parts):
                weights = jnp.exp2((scores - new_peak) * unit)
                total = total + jnp.sum(weights, axis=0, keepdims=True)
                stage_ref[slot, head] = weights.astype(jnp.bfloat16)
                mark_ref[slot, pl.ds(head, 1), :] = new_peak
            peak_ref[row, :] = new_peak
            total_ref[row, :] = total
            for _, slot in sides:
                copy_out(slot, head).start()

    if group == 1:
        visit(0, [(0, 0), (1, 1)])
        visit(1, [(0, 2), (1, 3)])
    else:
        for q_side, k_side, slot, condition in single_slots(group, spot_ref[1]):
            guarded(condition, functools.partial(visit, q_side, [(k_side, slot)]))

    def wait_all():
        for slot in range(weight_ref.shape[0]):
            for head in range(heads):
                copy_out(slot, head).wait()

    return wait_all


def rotate_keys(group, raw, cos_ref, sin_ref, key_ref):
    for side in range(CORES):
        cos_table = cos_ref[group * CORES + side]
        sin_table = sin_ref[group * CORES + side]
        for head in range(key_ref.shape[1]):
            key_ref[side, head] = rotated(raw(side, head), cos_table, sin_table)


def first_kernel(
    lengths_ref, spot_ref, cos_ref, sin_ref, k_all, k_other, q_all, v_all, got_ref,
    query_ref, value_ref, weight_ref, mark_ref, peak_ref, total_ref, key_ref, stage_ref, sent,
):
    heads, rows = k_other.shape[:2]
    core = spot_ref[1]
    for side in range(CORES):
        cos_table = cos_ref[side]
        sin_table = sin_ref[side]
        for head in range(2 * heads):
            raw = q_all[core * 2 * heads + head] if side == 0 else got_ref[head]
            query_ref[side, head // 2, pl.ds((head % 2) * rows, rows), :] = rotated(
                raw, cos_table, sin_table
            )

    def raw_key(side, head):
        return k_all[core * heads + head] if side == 0 else k_other[head]

    for head in range(heads):
        value_ref[head] = v_all[core * heads + head]
        value_ref[heads + head] = got_ref[2 * heads + head]
    rotate_keys(0, raw_key, cos_ref, sin_ref, key_ref)
    peak_ref[...] = jnp.full_like(peak_ref, masked)
    total_ref[...] = jnp.zeros_like(total_ref)
    gather_stats(
        0, lengths_ref, spot_ref, query_ref, lambda s, h: key_ref[s, h],
        weight_ref, mark_ref, peak_ref, total_ref, stage_ref, sent,
    )()


def next_kernel(
    lengths_ref, spot_ref, cos_ref, sin_ref, k_own, k_other, query_ref, old_peak, old_total,
    weight_ref, mark_ref, peak_ref, total_ref, key_ref, stage_ref, sent,
):
    raw = (k_own, k_other)
    rotate_keys(1, lambda side, head: raw[side][head], cos_ref, sin_ref, key_ref)
    peak_ref[...] = old_peak[...]
    total_ref[...] = old_total[...]
    gather_stats(
        1, lengths_ref, spot_ref, query_ref, lambda s, h: key_ref[s, h],
        weight_ref, mark_ref, peak_ref, total_ref, stage_ref, sent,
    )()


def last_kernel(
    lengths_ref, spot_ref, cos_ref, sin_ref, k_own, k_other, query_ref, old_peak, old_total,
    weight_ref, mark_ref, level_ref, squares_ref, peak_ref, total_ref, key_ref, stage_ref, sent,
):
    raw = (k_own, k_other)
    rotate_keys(2, lambda side, head: raw[side][head], cos_ref, sin_ref, key_ref)
    peak_ref[...] = old_peak[...]
    total_ref[...] = old_total[...]
    wait_all = gather_stats(
        2, lengths_ref, spot_ref, query_ref, lambda s, h: key_ref[s, h],
        weight_ref, mark_ref, peak_ref, total_ref, stage_ref, sent,
    )
    natural = peak_ref[...] * score_scale + jnp.log(total_ref[...])
    level_ref[...] = natural * log2_e
    squares = jnp.sum(natural * natural, axis=(0, 1), keepdims=True)
    squares_ref[...] = jnp.broadcast_to(squares, squares_ref.shape)
    wait_all()


def fetch(weight_ref, held_ref, ready):
    def copy(slot):
        return pltpu.make_async_copy(weight_ref.at[slot], held_ref.at[slot], ready.at[slot, 0])

    return copy


def weighed(weight_ref, mark_ref, level_ref, value, q_side, head, heads, slot):
    scale = jnp.exp2(
        mark_ref[slot, pl.ds(head, 1), :] * unit - level_ref[pl.ds(q_side * heads + head, 1), :]
    )
    return scale * lax.dot_general(
        value, weight_ref[slot, head], TN, preferred_element_type=jnp.float32
    )


def near_kernel(
    spot_ref, level_ref, weight_0, mark_0, weight_1, mark_1, v0_ref, v1_ref, sum_ref,
    held_0, held_1, ready_0, ready_1,
):
    heads = sum_ref.shape[1]
    copies_0 = fetch(weight_0, held_0, ready_0)
    copies_1 = fetch(weight_1, held_1, ready_1)
    for copy in (
        copies_0(0), copies_1(0), copies_1(1), copies_0(1), copies_1(2), copies_1(3), copies_0(2)
    ):
        copy.start()
    for q_side in range(CORES):
        for copy in (copies_0(q_side), copies_1(2 * q_side), copies_1(2 * q_side + 1)):
            copy.wait()
        for head in range(heads):
            part = functools.partial(weighed, q_side=q_side, head=head, heads=heads)
            sum_ref[q_side, head] = (
                part(held_0, mark_0, level_ref, v0_ref[q_side * heads + head], slot=q_side)
                + part(held_1, mark_1, level_ref, v1_ref[head], slot=2 * q_side)
                + part(held_1, mark_1, level_ref, v1_ref[heads + head], slot=2 * q_side + 1)
            )
    copies_0(2).wait()

    def cross(q_side, k_side, slot):
        for head in range(heads):
            sum_ref[q_side, head] += weighed(
                held_0, mark_0, level_ref, v0_ref[k_side * heads + head], q_side, head, heads, slot
            )

    for q_side, k_side, slot, condition in single_slots(0, spot_ref[1])[2:]:
        guarded(condition, functools.partial(cross, q_side, k_side, slot))


def far_kernel(
    side, spot_ref, level_ref, weight_2, mark_2, v2_ref, near_ref, out_ref,
    sum_ref, held, ready,
):
    heads = near_ref.shape[1]
    copies = fetch(weight_2, held, ready)
    cross_here = [entry for entry in single_slots(2, spot_ref[1])[2:] if entry[0] == side]
    for slot in (2, side):
        copies(slot).start()
    sum_ref[...] = near_ref[side]
    copies(2).wait()

    def cross(k_side, slot):
        for head in range(heads):
            sum_ref[head] += weighed(
                held, mark_2, level_ref, v2_ref[k_side * heads + head], side, head, heads, slot
            )

    for _, k_side, slot, condition in cross_here:
        guarded(condition, functools.partial(cross, k_side, slot))
    rows = out_ref.shape[1]
    copies(side).wait()
    for head in range(heads):
        block = sum_ref[head] + weighed(
            held, mark_2, level_ref, v2_ref[side * heads + head], side, head, heads, side
        )
        turned = jnp.transpose(block, (1, 0)).astype(jnp.bfloat16)
        out_ref[head * 2] = turned[:rows]
        out_ref[head * 2 + 1] = turned[rows:]


def call(kernel, out_shape, scalars, count, flops, scratch=(), far_in=(), far_out=()):
    def run(*operands):
        return pl.pallas_call(
            kernel,
            out_shape=out_shape,
            in_specs=[SMEM] * scalars
            + [HBM if i in far_in else VMEM for i in range(scalars, count)],
            out_specs=tuple(
                HBM if i in far_out else VMEM for i in range(len(out_shape))
            ),
            scratch_shapes=list(scratch),
            cost_estimate=pl.CostEstimate(flops=flops, bytes_accessed=0, transcendentals=0),
            compiler_params=pltpu.CompilerParams(vmem_limit_bytes=VMEM_LIMIT),
        )(*operands)

    return run


def by_head(tensor):
    return lax.optimization_barrier(jnp.transpose(tensor, (1, 0, 2)))


def half_of(tensor, core):
    part = tensor.shape[0] // CORES
    return jnp.where(core == 0, tensor[:part], tensor[part:])


def device_part(queries, keys, values, doc_lengths):
    rows, query_heads, width = queries.shape[1:]
    key_heads = keys.shape[2]
    heads = key_heads // CORES
    members = query_heads // key_heads
    devices = lax.axis_size(DP_SEQ)
    core = lax.axis_index("seq_2")
    chip = lax.axis_index(CHIP)
    f32, bf16 = jnp.float32, jnp.bfloat16
    shape = jax.ShapeDtypeStruct
    spot = jnp.stack([chip, core]).astype(jnp.int32)

    k_all = by_head(keys[0])
    k1_own = up_chip(half_of(k_all, core))
    k0_other = swapped(half_of(k_all, 1 - core))
    k1_other = up_chip(k0_other)
    k2_own = up_chip(k1_own)
    q_all = by_head(queries[0])
    v_all = by_head(values[0])
    give = jnp.concatenate([half_of(q_all, 1 - core), half_of(v_all, 1 - core)], axis=0)
    got = swapped(give)

    table = shape((3 * CORES, rows, width), f32)
    lane = jnp.arange(width // 2, dtype=f32)
    frequency = rope_base ** (-2.0 * lane / width)
    frequency = jnp.concatenate([frequency, frequency])[None, :]
    cos_table, sin_table = call(table_kernel, (table, table), 2, 3, TABLE_FLOPS)(
        doc_lengths, spot, frequency
    )
    k2_other = up_chip(k1_other)

    stats = shape((CORES * heads, members * rows), f32)
    q_shape = shape((CORES, heads, members * rows, width), bf16)
    key_scratch = pltpu.VMEM((CORES, heads, rows, width), bf16)

    def slots(count):
        return (
            pltpu.HBM((count, heads, rows, members * rows), bf16),
            shape((count, heads, members * rows), f32),
        )

    def staged(count):
        return (
            key_scratch,
            pltpu.VMEM((count, heads, rows, members * rows), bf16),
            pltpu.SemaphoreType.DMA((count, heads)),
        )

    v_shape = shape((CORES * heads, rows, width), bf16)
    query_rot, v0, weight_0, mark_0, peak, total = call(
        first_kernel, (q_shape, v_shape, *slots(3), stats, stats), 2, 9, FIRST_FLOPS,
        staged(3), far_out=(2,),
    )(doc_lengths, spot, cos_table, sin_table, k_all, k0_other, q_all, v_all, got)
    v1 = up_chip(v0)
    v2 = up_chip(v1)
    weight_1, mark_1, peak, total = call(
        next_kernel, (*slots(4), stats, stats), 2, 9, NEXT_FLOPS, staged(4),
        far_out=(0,),
    )(doc_lengths, spot, cos_table, sin_table, k1_own, k1_other, query_rot, peak, total)
    weight_2, mark_2, level, squares = call(
        last_kernel,
        (*slots(3), stats, shape((lax.axis_size(("seq_1", "seq_2")), width), f32)),
        2,
        9,
        NEXT_FLOPS,
        (pltpu.VMEM(stats.shape, f32), pltpu.VMEM(stats.shape, f32), *staged(3)),
        far_out=(0,),
    )(doc_lengths, spot, cos_table, sin_table, k2_own, k2_other, query_rot, peak, total)
    squares = lax.all_to_all(squares, ("seq_1", "seq_2"), 0, 0)
    across = ("dp_0", "dp_1", "seq_0")
    squares = jnp.sum(squares, axis=0, keepdims=True)
    squares = jnp.broadcast_to(squares, (lax.axis_size(across), width))
    squares = lax.all_to_all(squares, across, 0, 0)
    squares = jnp.sum(squares, axis=0, keepdims=True)
    z_loss = squares[0, 0] / (devices * rows * query_heads)

    weight_0, weight_1, weight_2 = (
        pltpu.with_memory_space_constraint(array, pltpu.HBM)
        for array in (weight_0, weight_1, weight_2)
    )
    sum_shape = shape((CORES, heads, width, members * rows), f32)
    (near,) = call(
        near_kernel, (sum_shape,), 1, 8, NEAR_FLOPS,
        (*staged(3)[1:2], *staged(4)[1:2], *staged(3)[2:], *staged(4)[2:]),
        far_in=(2, 4),
    )(spot, level, weight_0, mark_0, weight_1, mark_1, v0, v1)
    out_shape = shape((heads * members, rows, width), bf16)
    own, other = (
        call(
            functools.partial(far_kernel, side), (out_shape,), 1, 6, NEAR_FLOPS,
            (pltpu.VMEM(sum_shape.shape[1:], f32), *staged(3)[1:]),
            far_in=(2,),
        )(spot, level, weight_2, mark_2, v2, near)[0]
        for side in range(2)
    )
    partner = swapped(other)
    low = jnp.where(core == 0, own, partner)
    high = jnp.where(core == 0, partner, own)
    attended = jnp.transpose(jnp.concatenate([low, high], axis=0), (1, 0, 2))
    return (attended[None], z_loss)


VMEM_LIMIT = 20 * 1024 * 1024
TABLE_FLOPS = 4_000_000
FIRST_FLOPS = 6_000_000
NEXT_FLOPS = 6_000_000
NEAR_FLOPS = 3_000_000


def solution(mesh):
    torus = Mesh(mesh.devices.reshape(8, 2, 2, 8, 2), ("dp_0", "dp_1", "seq_0", "seq_1", "seq_2"))
    in_specs = (P(DP, SEQ, None, None), P(DP, SEQ, None, None), P(DP, SEQ, None, None), P(DP, None))
    out_specs = (P(DP, SEQ, None, None), P())
    return jax.shard_map(
        device_part, mesh=torus, in_specs=in_specs, out_specs=out_specs, check_vma=False
    )
```

```python
import functools
import math

import jax
import jax.numpy as jnp
from jax import lax
from jax.experimental import pallas as pl
from jax.experimental.pallas import tpu as pltpu
from jax.sharding import Mesh
from jax.sharding import PartitionSpec as P

WINDOW = 1024
SEQ = ("seq_0", "seq_1", "seq_2")
CHIP = ("seq_0", "seq_1")
DP_SEQ = ("dp_0", "dp_1", "seq_0", "seq_1", "seq_2")
DP = ("dp_0", "dp_1")
CORES = 2


rope_base = 500000.0
score_scale = 1.0 / 12.0
masked = -1e30
log2_e = 1.0 / math.log(2.0)
unit = score_scale * log2_e

VMEM = pl.BlockSpec(memory_space=pltpu.VMEM)
SMEM = pl.BlockSpec(memory_space=pltpu.SMEM)
HBM = pl.BlockSpec(memory_space=pltpu.HBM)
NT = (((1,), (1,)), ((), ()))
TN = (((0,), (0,)), ((), ()))


def up_chip(block, chips=1):
    count = lax.axis_size(SEQ)
    step = chips * CORES
    return lax.ppermute(block, SEQ, [(i, i + step) for i in range(count - step)])


def swapped(block):
    return lax.ppermute(block, "seq_2", [(0, 1), (1, 0)])


def rotated(block, cos_table, sin_table):
    wide = block.astype(jnp.float32)
    half = wide.shape[-1] // 2
    return (wide * cos_table + pltpu.roll(wide, half, 1) * sin_table).astype(jnp.bfloat16)


def doc_ends(lengths_ref):
    ends = [lengths_ref[0, 0]]
    for i in range(1, lengths_ref.shape[1]):
        ends.append(ends[-1] + lengths_ref[0, i])
    return ends


def doc_start(ends, at, low):
    for end in ends:
        low = jnp.maximum(low, jnp.where(at >= end, end, 0))
    return low


def block_start(spot_ref, rows, group, parity):
    core = spot_ref[1]
    place = core if parity == 0 else 1 - core
    return ((spot_ref[0] - group) * CORES + place) * rows


def single_slots(group, core):
    flip = core if group == 0 else 1 - core
    return [(0, 0, 0, None), (1, 1, 1, None), (0, 1, 2, flip == 1), (1, 0, 2, flip == 0)]


def guarded(condition, body):
    if condition is None:
        body()
    else:
        pl.when(condition)(body)


def cos_sin(angles):
    turns = jnp.floor(angles * (2.0 / math.pi) + 0.5)
    rest = ((angles - turns * 1.5703125) - turns * 4.837512969970703125e-4) - turns * 7.54978995489188216e-8
    square = rest * rest
    sine = (
        (-1.9515295891e-4 * square + 8.3321608736e-3) * square - 1.6666654611e-1
    ) * square * rest + rest
    cosine = (
        (2.443315711809948e-5 * square - 1.388731625493765e-3) * square + 4.166664568298827e-2
    ) * square * square - 0.5 * square + 1.0
    quarter = turns.astype(jnp.int32)
    odd = (quarter & 1) == 1
    return (
        jnp.where(((quarter + 1) & 2) == 2, -1.0, 1.0) * jnp.where(odd, sine, cosine),
        jnp.where((quarter & 2) == 2, -1.0, 1.0) * jnp.where(odd, cosine, sine),
    )


def table_kernel(lengths_ref, spot_ref, frequency_ref, cos_ref, sin_ref):
    rows, width = cos_ref.shape[1:]
    half = width // 2
    pairs = rows // 2
    ends = doc_ends(lengths_ref)
    upper = lax.broadcasted_iota(jnp.int32, (pairs, width), 1) >= half
    sign = jnp.where(upper, 1.0, -1.0)
    frequency = frequency_ref[...]
    for index in range(cos_ref.shape[0]):
        begin = block_start(spot_ref, rows, index // CORES, index % CORES)
        at = begin + lax.broadcasted_iota(jnp.int32, (pairs, width), 0)
        at = at + jnp.where(upper, pairs, 0)
        places = at - doc_start(ends, at, jnp.zeros_like(at))
        cosine, sine = cos_sin(places.astype(jnp.float32) * frequency)
        for out_ref, table, factor in ((cos_ref, cosine, None), (sin_ref, sine, sign)):
            turned = pltpu.roll(table, half, 1)
            first = jnp.where(upper, turned, table)
            second = jnp.where(upper, table, turned)
            if factor is not None:
                first = first * factor
                second = second * factor
            out_ref[index, pl.ds(0, pairs), :] = first
            out_ref[index, pl.ds(pairs, pairs), :] = second


def bias_of(ends, spot_ref, rows, group, q_side, k_side):
    query_at = block_start(spot_ref, rows, 0, q_side) + lax.broadcasted_iota(
        jnp.int32, (1, rows), 1
    )
    key_at = block_start(spot_ref, rows, group, k_side) + lax.broadcasted_iota(
        jnp.int32, (rows, rows), 0
    )
    low = doc_start(ends, query_at, jnp.maximum(query_at - (WINDOW - 1), 0))
    bias = jnp.where((key_at >= low) & (key_at <= query_at), 0.0, masked)
    return jnp.concatenate([bias, bias], axis=1)


def gather_stats(
    group, lengths_ref, spot_ref, query_ref, key_of, weight_ref, mark_ref, peak_ref, total_ref,
    stage_ref, sent,
):
    heads = query_ref.shape[1]
    rows = weight_ref.shape[2]
    ends = doc_ends(lengths_ref)

    def copy_out(slot, head):
        return pltpu.make_async_copy(
            stage_ref.at[slot, head], weight_ref.at[slot, head], sent.at[slot, head]
        )

    def visit(q_side, sides):
        biases = [bias_of(ends, spot_ref, rows, group, q_side, k_side) for k_side, _ in sides]

        def scored(head):
            return [
                lax.dot_general(
                    key_of(k_side, head),
                    query_ref[q_side, head],
                    NT,
                    preferred_element_type=jnp.float32,
                )
                + bias
                for (k_side, _), bias in zip(sides, biases)
            ]

        for head in range(heads):
            parts = scored(head)
            row = pl.ds(q_side * heads + head, 1)
            old_peak = peak_ref[row, :]
            new_peak = old_peak
            for scores in parts:
                new_peak = jnp.maximum(new_peak, jnp.max(scores, axis=0, keepdims=True))
            total = total_ref[row, :] * jnp.exp2((old_peak - new_peak) * unit)
            for (_, slot), scores in zip(sides, parts):
                weights = jnp.exp2((scores - new_peak) * unit)
                total = total + jnp.sum(weights, axis=0, keepdims=True)
                stage_ref[slot, head] = weights.astype(jnp.bfloat16)
                mark_ref[slot, pl.ds(head, 1), :] = new_peak
            peak_ref[row, :] = new_peak
            total_ref[row, :] = total
            for _, slot in sides:
                copy_out(slot, head).start()

    if group == 1:
        visit(0, [(0, 0), (1, 1)])
        visit(1, [(0, 2), (1, 3)])
    else:
        for q_side, k_side, slot, condition in single_slots(group, spot_ref[1]):
            guarded(condition, functools.partial(visit, q_side, [(k_side, slot)]))

    def wait_all():
        for slot in range(weight_ref.shape[0]):
            for head in range(heads):
                copy_out(slot, head).wait()

    return wait_all


def rotate_keys(group, raw, cos_ref, sin_ref, key_ref):
    for side in range(CORES):
        cos_table = cos_ref[group * CORES + side]
        sin_table = sin_ref[group * CORES + side]
        for head in range(key_ref.shape[1]):
            key_ref[side, head] = rotated(raw(side, head), cos_table, sin_table)


def first_kernel(
    lengths_ref, spot_ref, cos_ref, sin_ref, k_all, k_other, q_all, v_all, got_ref,
    query_ref, value_ref, weight_ref, mark_ref, peak_ref, total_ref, key_ref, stage_ref, sent,
):
    heads, rows = k_other.shape[:2]
    core = spot_ref[1]
    for side in range(CORES):
        cos_table = cos_ref[side]
        sin_table = sin_ref[side]
        for head in range(2 * heads):
            raw = q_all[core * 2 * heads + head] if side == 0 else got_ref[head]
            query_ref[side, head // 2, pl.ds((head % 2) * rows, rows), :] = rotated(
                raw, cos_table, sin_table
            )

    def raw_key(side, head):
        return k_all[core * heads + head] if side == 0 else k_other[head]

    for head in range(heads):
        value_ref[head] = v_all[core * heads + head]
        value_ref[heads + head] = got_ref[2 * heads + head]
    rotate_keys(0, raw_key, cos_ref, sin_ref, key_ref)
    peak_ref[...] = jnp.full_like(peak_ref, masked)
    total_ref[...] = jnp.zeros_like(total_ref)
    gather_stats(
        0, lengths_ref, spot_ref, query_ref, lambda s, h: key_ref[s, h],
        weight_ref, mark_ref, peak_ref, total_ref, stage_ref, sent,
    )()


def next_kernel(
    lengths_ref, spot_ref, cos_ref, sin_ref, k_own, k_other, query_ref, old_peak, old_total,
    weight_ref, mark_ref, peak_ref, total_ref, key_ref, stage_ref, sent,
):
    raw = (k_own, k_other)
    rotate_keys(1, lambda side, head: raw[side][head], cos_ref, sin_ref, key_ref)
    peak_ref[...] = old_peak[...]
    total_ref[...] = old_total[...]
    gather_stats(
        1, lengths_ref, spot_ref, query_ref, lambda s, h: key_ref[s, h],
        weight_ref, mark_ref, peak_ref, total_ref, stage_ref, sent,
    )()


def last_kernel(
    lengths_ref, spot_ref, cos_ref, sin_ref, k_own, k_other, query_ref, old_peak, old_total,
    weight_ref, mark_ref, level_ref, squares_ref, peak_ref, total_ref, key_ref, stage_ref, sent,
):
    raw = (k_own, k_other)
    rotate_keys(2, lambda side, head: raw[side][head], cos_ref, sin_ref, key_ref)
    peak_ref[...] = old_peak[...]
    total_ref[...] = old_total[...]
    wait_all = gather_stats(
        2, lengths_ref, spot_ref, query_ref, lambda s, h: key_ref[s, h],
        weight_ref, mark_ref, peak_ref, total_ref, stage_ref, sent,
    )
    natural = peak_ref[...] * score_scale + jnp.log(total_ref[...])
    level_ref[...] = natural * log2_e
    squares = jnp.sum(natural * natural, axis=(0, 1), keepdims=True)
    squares_ref[...] = jnp.broadcast_to(squares, squares_ref.shape)
    wait_all()


def fetch(weight_ref, held_ref, ready):
    def copy(slot):
        return pltpu.make_async_copy(weight_ref.at[slot], held_ref.at[slot], ready.at[slot, 0])

    return copy


def weighed(weight_ref, mark_ref, level_ref, value, q_side, head, heads, slot):
    scale = jnp.exp2(
        mark_ref[slot, pl.ds(head, 1), :] * unit - level_ref[pl.ds(q_side * heads + head, 1), :]
    )
    return scale * lax.dot_general(
        value, weight_ref[slot, head], TN, preferred_element_type=jnp.float32
    )


def near_kernel(
    spot_ref, level_ref, weight_0, mark_0, weight_1, mark_1, v0_ref, v1_ref, own_ref, other_ref,
    held_0, held_1, ready_0, ready_1,
):
    heads = own_ref.shape[0]
    sums = (own_ref, other_ref)
    copies_0 = fetch(weight_0, held_0, ready_0)
    copies_1 = fetch(weight_1, held_1, ready_1)
    for copy in (
        copies_0(0), copies_1(0), copies_1(1), copies_0(1), copies_1(2), copies_1(3), copies_0(2)
    ):
        copy.start()
    for q_side in range(CORES):
        for copy in (copies_0(q_side), copies_1(2 * q_side), copies_1(2 * q_side + 1)):
            copy.wait()
        for head in range(heads):
            part = functools.partial(weighed, q_side=q_side, head=head, heads=heads)
            sums[q_side][head] = (
                part(held_0, mark_0, level_ref, v0_ref[q_side * heads + head], slot=q_side)
                + part(held_1, mark_1, level_ref, v1_ref[head], slot=2 * q_side)
                + part(held_1, mark_1, level_ref, v1_ref[heads + head], slot=2 * q_side + 1)
            )
    copies_0(2).wait()

    def cross(q_side, k_side, slot):
        for head in range(heads):
            sums[q_side][head] += weighed(
                held_0, mark_0, level_ref, v0_ref[k_side * heads + head], q_side, head, heads, slot
            )

    for q_side, k_side, slot, condition in single_slots(0, spot_ref[1])[2:]:
        guarded(condition, functools.partial(cross, q_side, k_side, slot))


def far_kernel(
    side, spot_ref, level_ref, weight_2, mark_2, v2_ref, near_ref, out_ref, sum_ref, held, ready
):
    heads, rows = near_ref.shape[0], out_ref.shape[1]
    copies = fetch(weight_2, held, ready)
    crossed = spot_ref[1] == side
    copies(side).start()

    @pl.when(crossed)
    def _():
        copies(2).start()

    copies(side).wait()

    def summed(head):
        return near_ref[head] + weighed(
            held, mark_2, level_ref, v2_ref[side * heads + head], side, head, heads, side
        )

    def write(head, block):
        turned = jnp.transpose(block, (1, 0)).astype(jnp.bfloat16)
        out_ref[head * 2] = turned[:rows]
        out_ref[head * 2 + 1] = turned[rows:]

    @pl.when(crossed)
    def _():
        for head in range(heads):
            sum_ref[head] = summed(head)
        copies(2).wait()
        for head in range(heads):
            write(
                head,
                sum_ref[head]
                + weighed(
                    held, mark_2, level_ref, v2_ref[(1 - side) * heads + head],
                    side, head, heads, 2,
                ),
            )

    @pl.when(jnp.logical_not(crossed))
    def _():
        for head in range(heads):
            write(head, summed(head))


def call(kernel, out_shape, scalars, count, flops, scratch=(), far_in=(), far_out=()):
    def run(*operands):
        return pl.pallas_call(
            kernel,
            out_shape=out_shape,
            in_specs=[SMEM] * scalars
            + [HBM if i in far_in else VMEM for i in range(scalars, count)],
            out_specs=tuple(
                HBM if i in far_out else VMEM for i in range(len(out_shape))
            ),
            scratch_shapes=list(scratch),
            cost_estimate=pl.CostEstimate(flops=flops, bytes_accessed=0, transcendentals=0),
            compiler_params=pltpu.CompilerParams(vmem_limit_bytes=VMEM_LIMIT),
        )(*operands)

    return run


def by_head(tensor):
    return lax.optimization_barrier(jnp.transpose(tensor, (1, 0, 2)))


def half_of(tensor, core):
    part = tensor.shape[0] // CORES
    return jnp.where(core == 0, tensor[:part], tensor[part:])


def device_part(queries, keys, values, doc_lengths):
    rows, query_heads, width = queries.shape[1:]
    key_heads = keys.shape[2]
    heads = key_heads // CORES
    members = query_heads // key_heads
    devices = lax.axis_size(DP_SEQ)
    core = lax.axis_index("seq_2")
    chip = lax.axis_index(CHIP)
    f32, bf16 = jnp.float32, jnp.bfloat16
    shape = jax.ShapeDtypeStruct
    spot = jnp.stack([chip, core]).astype(jnp.int32)

    k_all = by_head(keys[0])
    k1_own = up_chip(half_of(k_all, core))
    k0_other = swapped(half_of(k_all, 1 - core))
    k1_other = up_chip(k0_other)
    k2_own = up_chip(k1_own)
    q_all = by_head(queries[0])
    v_all = by_head(values[0])
    give = jnp.concatenate([half_of(q_all, 1 - core), half_of(v_all, 1 - core)], axis=0)
    got = swapped(give)

    table = shape((3 * CORES, rows, width), f32)
    lane = jnp.arange(width // 2, dtype=f32)
    frequency = rope_base ** (-2.0 * lane / width)
    frequency = jnp.concatenate([frequency, frequency])[None, :]
    cos_table, sin_table = call(table_kernel, (table, table), 2, 3, TABLE_FLOPS)(
        doc_lengths, spot, frequency
    )
    k2_other = up_chip(k1_other)

    stats = shape((CORES * heads, members * rows), f32)
    q_shape = shape((CORES, heads, members * rows, width), bf16)
    key_scratch = pltpu.VMEM((CORES, heads, rows, width), bf16)

    def slots(count):
        return (
            pltpu.HBM((count, heads, rows, members * rows), bf16),
            shape((count, heads, members * rows), f32),
        )

    def staged(count):
        return (
            key_scratch,
            pltpu.VMEM((count, heads, rows, members * rows), bf16),
            pltpu.SemaphoreType.DMA((count, heads)),
        )

    v_shape = shape((CORES * heads, rows, width), bf16)
    query_rot, v0, weight_0, mark_0, peak, total = call(
        first_kernel, (q_shape, v_shape, *slots(3), stats, stats), 2, 9, FIRST_FLOPS,
        staged(3), far_out=(2,),
    )(doc_lengths, spot, cos_table, sin_table, k_all, k0_other, q_all, v_all, got)
    v1 = up_chip(v0)
    v2 = up_chip(v1)
    weight_1, mark_1, peak, total = call(
        next_kernel, (*slots(4), stats, stats), 2, 9, NEXT_FLOPS, staged(4),
        far_out=(0,),
    )(doc_lengths, spot, cos_table, sin_table, k1_own, k1_other, query_rot, peak, total)
    weight_2, mark_2, level, squares = call(
        last_kernel,
        (*slots(3), stats, shape((lax.axis_size(("seq_1", "seq_2")), width), f32)),
        2,
        9,
        NEXT_FLOPS,
        (pltpu.VMEM(stats.shape, f32), pltpu.VMEM(stats.shape, f32), *staged(3)),
        far_out=(0,),
    )(doc_lengths, spot, cos_table, sin_table, k2_own, k2_other, query_rot, peak, total)
    squares = lax.all_to_all(squares, ("seq_1", "seq_2"), 0, 0)
    across = ("dp_0", "dp_1", "seq_0")
    squares = jnp.sum(squares, axis=0, keepdims=True)
    squares = jnp.broadcast_to(squares, (lax.axis_size(across), width))
    squares = lax.all_to_all(squares, across, 0, 0)
    squares = jnp.sum(squares, axis=0, keepdims=True)
    z_loss = squares[0, 0] / (devices * rows * query_heads)

    weight_0, weight_1, weight_2 = (
        pltpu.with_memory_space_constraint(array, pltpu.HBM)
        for array in (weight_0, weight_1, weight_2)
    )
    sum_shape = shape((heads, width, members * rows), f32)
    near = call(
        near_kernel, (sum_shape, sum_shape), 1, 8, NEAR_FLOPS,
        (*staged(3)[1:2], *staged(4)[1:2], *staged(3)[2:], *staged(4)[2:]),
        far_in=(2, 4),
    )(spot, level, weight_0, mark_0, weight_1, mark_1, v0, v1)
    out_shape = shape((heads * members, rows, width), bf16)
    own, other = (
        call(
            functools.partial(far_kernel, side), (out_shape,), 1, 6, NEAR_FLOPS,
            (pltpu.VMEM(sum_shape.shape, f32), *staged(3)[1:]),
            far_in=(2,),
        )(spot, level, weight_2, mark_2, v2, near[side])[0]
        for side in range(2)
    )
    partner = swapped(other)
    low = jnp.where(core == 0, own, partner)
    high = jnp.where(core == 0, partner, own)
    attended = jnp.transpose(jnp.concatenate([low, high], axis=0), (1, 0, 2))
    return (attended[None], z_loss)


VMEM_LIMIT = 20 * 1024 * 1024
TABLE_FLOPS = 4_000_000
FIRST_FLOPS = 6_000_000
NEXT_FLOPS = 6_000_000
NEAR_FLOPS = 3_000_000


def solution(mesh):
    torus = Mesh(mesh.devices.reshape(8, 2, 2, 8, 2), ("dp_0", "dp_1", "seq_0", "seq_1", "seq_2"))
    in_specs = (P(DP, SEQ, None, None), P(DP, SEQ, None, None), P(DP, SEQ, None, None), P(DP, None))
    out_specs = (P(DP, SEQ, None, None), P())
    return jax.shard_map(
        device_part, mesh=torus, in_specs=in_specs, out_specs=out_specs, check_vma=False
    )
```

```python
import functools
import math

import jax
import jax.numpy as jnp
from jax import lax
from jax.experimental import pallas as pl
from jax.experimental.pallas import tpu as pltpu
from jax.sharding import Mesh
from jax.sharding import PartitionSpec as P

WINDOW = 1024
SEQ = ("seq_0", "seq_1", "seq_2")
CHIP = ("seq_0", "seq_1")
DP_SEQ = ("dp_0", "dp_1", "seq_0", "seq_1", "seq_2")
DP = ("dp_0", "dp_1")
CORES = 2


rope_base = 500000.0
score_scale = 1.0 / 12.0
masked = -1e30
log2_e = 1.0 / math.log(2.0)
unit = score_scale * log2_e

VMEM = pl.BlockSpec(memory_space=pltpu.VMEM)
SMEM = pl.BlockSpec(memory_space=pltpu.SMEM)
HBM = pl.BlockSpec(memory_space=pltpu.HBM)
NT = (((1,), (1,)), ((), ()))
TN = (((0,), (0,)), ((), ()))


def up_chip(block, chips=1):
    count = lax.axis_size(SEQ)
    step = chips * CORES
    return lax.ppermute(block, SEQ, [(i, i + step) for i in range(count - step)])


def swapped(block):
    return lax.ppermute(block, "seq_2", [(0, 1), (1, 0)])


def rotated(block, cos_table, sin_table):
    wide = block.astype(jnp.float32)
    half = wide.shape[-1] // 2
    return (wide * cos_table + pltpu.roll(wide, half, 1) * sin_table).astype(jnp.bfloat16)


def doc_ends(lengths_ref):
    ends = [lengths_ref[0, 0]]
    for i in range(1, lengths_ref.shape[1]):
        ends.append(ends[-1] + lengths_ref[0, i])
    return ends


def doc_start(ends, at, low):
    for end in ends:
        low = jnp.maximum(low, jnp.where(at >= end, end, 0))
    return low


def block_start(spot_ref, rows, group, parity):
    core = spot_ref[1]
    place = core if parity == 0 else 1 - core
    return ((spot_ref[0] - group) * CORES + place) * rows


def single_slots(group, core):
    flip = core if group == 0 else 1 - core
    return [(0, 0, 0, None), (1, 1, 1, None), (0, 1, 2, flip == 1), (1, 0, 2, flip == 0)]


def guarded(condition, body):
    if condition is None:
        body()
    else:
        pl.when(condition)(body)


def cos_sin(angles):
    turns = jnp.floor(angles * (2.0 / math.pi) + 0.5)
    rest = ((angles - turns * 1.5703125) - turns * 4.837512969970703125e-4) - turns * 7.54978995489188216e-8
    square = rest * rest
    sine = (
        (-1.9515295891e-4 * square + 8.3321608736e-3) * square - 1.6666654611e-1
    ) * square * rest + rest
    cosine = (
        (2.443315711809948e-5 * square - 1.388731625493765e-3) * square + 4.166664568298827e-2
    ) * square * square - 0.5 * square + 1.0
    quarter = turns.astype(jnp.int32)
    odd = (quarter & 1) == 1
    return (
        jnp.where(((quarter + 1) & 2) == 2, -1.0, 1.0) * jnp.where(odd, sine, cosine),
        jnp.where((quarter & 2) == 2, -1.0, 1.0) * jnp.where(odd, cosine, sine),
    )


def table_kernel(lengths_ref, spot_ref, frequency_ref, cos_ref, sin_ref):
    rows, width = cos_ref.shape[1:]
    half = width // 2
    pairs = rows // 2
    ends = doc_ends(lengths_ref)
    upper = lax.broadcasted_iota(jnp.int32, (pairs, width), 1) >= half
    sign = jnp.where(upper, 1.0, -1.0)
    frequency = frequency_ref[...]
    for index in range(cos_ref.shape[0]):
        begin = block_start(spot_ref, rows, index // CORES, index % CORES)
        at = begin + lax.broadcasted_iota(jnp.int32, (pairs, width), 0)
        at = at + jnp.where(upper, pairs, 0)
        places = at - doc_start(ends, at, jnp.zeros_like(at))
        cosine, sine = cos_sin(places.astype(jnp.float32) * frequency)
        for out_ref, table, factor in ((cos_ref, cosine, None), (sin_ref, sine, sign)):
            turned = pltpu.roll(table, half, 1)
            first = jnp.where(upper, turned, table)
            second = jnp.where(upper, table, turned)
            if factor is not None:
                first = first * factor
                second = second * factor
            out_ref[index, pl.ds(0, pairs), :] = first
            out_ref[index, pl.ds(pairs, pairs), :] = second


def bias_of(ends, spot_ref, rows, group, q_side, k_side):
    query_at = block_start(spot_ref, rows, 0, q_side) + lax.broadcasted_iota(
        jnp.int32, (1, rows), 1
    )
    key_at = block_start(spot_ref, rows, group, k_side) + lax.broadcasted_iota(
        jnp.int32, (rows, rows), 0
    )
    low = doc_start(ends, query_at, jnp.maximum(query_at - (WINDOW - 1), 0))
    bias = jnp.where((key_at >= low) & (key_at <= query_at), 0.0, masked)
    return jnp.concatenate([bias, bias], axis=1)


def gather_stats(
    group, lengths_ref, spot_ref, query_ref, key_of, weight_ref, mark_ref, peak_ref, total_ref,
    stage_ref, sent,
):
    heads = query_ref.shape[1]
    rows = weight_ref.shape[2]
    ends = doc_ends(lengths_ref)

    def copy_out(slot, head):
        return pltpu.make_async_copy(
            stage_ref.at[slot, head], weight_ref.at[slot, head], sent.at[slot, head]
        )

    def visit(q_side, sides):
        biases = [bias_of(ends, spot_ref, rows, group, q_side, k_side) for k_side, _ in sides]

        def scored(head):
            return [
                lax.dot_general(
                    key_of(k_side, head),
                    query_ref[q_side, head],
                    NT,
                    preferred_element_type=jnp.float32,
                )
                + bias
                for (k_side, _), bias in zip(sides, biases)
            ]

        for head in range(heads):
            parts = scored(head)
            row = pl.ds(q_side * heads + head, 1)
            old_peak = peak_ref[row, :]
            new_peak = old_peak
            for scores in parts:
                new_peak = jnp.maximum(new_peak, jnp.max(scores, axis=0, keepdims=True))
            total = total_ref[row, :] * jnp.exp2((old_peak - new_peak) * unit)
            for (_, slot), scores in zip(sides, parts):
                weights = jnp.exp2((scores - new_peak) * unit)
                total = total + jnp.sum(weights, axis=0, keepdims=True)
                stage_ref[slot, head] = weights.astype(jnp.bfloat16)
                mark_ref[slot, pl.ds(head, 1), :] = new_peak
            peak_ref[row, :] = new_peak
            total_ref[row, :] = total
            for _, slot in sides:
                copy_out(slot, head).start()

    if group == 1:
        visit(0, [(0, 0), (1, 1)])
        visit(1, [(0, 2), (1, 3)])
    else:
        for q_side, k_side, slot, condition in single_slots(group, spot_ref[1]):
            guarded(condition, functools.partial(visit, q_side, [(k_side, slot)]))

    def wait_all():
        for slot in range(weight_ref.shape[0]):
            for head in range(heads):
                copy_out(slot, head).wait()

    return wait_all


def rotate_keys(group, raw, cos_ref, sin_ref, key_ref):
    for side in range(CORES):
        cos_table = cos_ref[group * CORES + side]
        sin_table = sin_ref[group * CORES + side]
        for head in range(key_ref.shape[1]):
            key_ref[side, head] = rotated(raw(side, head), cos_table, sin_table)


def first_kernel(
    lengths_ref, spot_ref, cos_ref, sin_ref, k_all, k_other, q_all, v_all, got_ref,
    query_ref, value_ref, weight_ref, mark_ref, peak_ref, total_ref, key_ref, stage_ref, sent,
):
    heads, rows = k_other.shape[:2]
    core = spot_ref[1]
    for side in range(CORES):
        cos_table = cos_ref[side]
        sin_table = sin_ref[side]
        for head in range(2 * heads):
            raw = q_all[core * 2 * heads + head] if side == 0 else got_ref[head]
            query_ref[side, head // 2, pl.ds((head % 2) * rows, rows), :] = rotated(
                raw, cos_table, sin_table
            )

    def raw_key(side, head):
        return k_all[core * heads + head] if side == 0 else k_other[head]

    for head in range(heads):
        value_ref[head] = v_all[core * heads + head]
        value_ref[heads + head] = got_ref[2 * heads + head]
    rotate_keys(0, raw_key, cos_ref, sin_ref, key_ref)
    peak_ref[...] = jnp.full_like(peak_ref, masked)
    total_ref[...] = jnp.zeros_like(total_ref)
    gather_stats(
        0, lengths_ref, spot_ref, query_ref, lambda s, h: key_ref[s, h],
        weight_ref, mark_ref, peak_ref, total_ref, stage_ref, sent,
    )()


def next_kernel(
    lengths_ref, spot_ref, cos_ref, sin_ref, k_own, k_other, query_ref, old_peak, old_total,
    weight_ref, mark_ref, peak_ref, total_ref, key_ref, stage_ref, sent,
):
    raw = (k_own, k_other)
    rotate_keys(1, lambda side, head: raw[side][head], cos_ref, sin_ref, key_ref)
    peak_ref[...] = old_peak[...]
    total_ref[...] = old_total[...]
    gather_stats(
        1, lengths_ref, spot_ref, query_ref, lambda s, h: key_ref[s, h],
        weight_ref, mark_ref, peak_ref, total_ref, stage_ref, sent,
    )()


def last_kernel(
    lengths_ref, spot_ref, cos_ref, sin_ref, k_own, k_other, query_ref, old_peak, old_total,
    weight_ref, mark_ref, level_ref, squares_ref, peak_ref, total_ref, key_ref, stage_ref, sent,
):
    raw = (k_own, k_other)
    rotate_keys(2, lambda side, head: raw[side][head], cos_ref, sin_ref, key_ref)
    peak_ref[...] = old_peak[...]
    total_ref[...] = old_total[...]
    wait_all = gather_stats(
        2, lengths_ref, spot_ref, query_ref, lambda s, h: key_ref[s, h],
        weight_ref, mark_ref, peak_ref, total_ref, stage_ref, sent,
    )
    natural = peak_ref[...] * score_scale + jnp.log(total_ref[...])
    level_ref[...] = natural * log2_e
    squares = jnp.sum(natural * natural, axis=(0, 1), keepdims=True)
    squares_ref[...] = jnp.broadcast_to(squares, squares_ref.shape)
    wait_all()


def fetch(weight_ref, held_ref, ready):
    def copy(slot):
        return pltpu.make_async_copy(weight_ref.at[slot], held_ref.at[slot], ready.at[slot, 0])

    return copy


def weighed(weight_ref, mark_ref, level_ref, value, q_side, head, heads, slot):
    scale = jnp.exp2(
        mark_ref[slot, pl.ds(head, 1), :] * unit - level_ref[pl.ds(q_side * heads + head, 1), :]
    )
    return scale * lax.dot_general(
        value, weight_ref[slot, head], TN, preferred_element_type=jnp.float32
    )


def near_kernel(
    spot_ref, level_ref, weight_0, mark_0, weight_1, mark_1, v0_ref, v1_ref, own_ref, other_ref,
    held_0, held_1, ready_0, ready_1,
):
    heads = own_ref.shape[0]
    sums = (own_ref, other_ref)
    copies_0 = fetch(weight_0, held_0, ready_0)
    copies_1 = fetch(weight_1, held_1, ready_1)
    for copy in (
        copies_0(0), copies_1(0), copies_1(1), copies_0(1), copies_1(2), copies_1(3), copies_0(2)
    ):
        copy.start()
    for q_side in range(CORES):
        for copy in (copies_0(q_side), copies_1(2 * q_side), copies_1(2 * q_side + 1)):
            copy.wait()
        for head in range(heads):
            part = functools.partial(weighed, q_side=q_side, head=head, heads=heads)
            sums[q_side][head] = (
                part(held_0, mark_0, level_ref, v0_ref[q_side * heads + head], slot=q_side)
                + part(held_1, mark_1, level_ref, v1_ref[head], slot=2 * q_side)
                + part(held_1, mark_1, level_ref, v1_ref[heads + head], slot=2 * q_side + 1)
            )
    copies_0(2).wait()

    def cross(q_side, k_side, slot):
        for head in range(heads):
            sums[q_side][head] += weighed(
                held_0, mark_0, level_ref, v0_ref[k_side * heads + head], q_side, head, heads, slot
            )

    for q_side, k_side, slot, condition in single_slots(0, spot_ref[1])[2:]:
        guarded(condition, functools.partial(cross, q_side, k_side, slot))


def far_kernel(
    side, spot_ref, level_ref, weight_2, mark_2, v2_ref, near_ref, out_ref, sum_ref, held, ready
):
    heads, rows = near_ref.shape[0], out_ref.shape[1]
    copies = fetch(weight_2, held, ready)
    crossed = spot_ref[1] == side
    lead, rest = pl.ds(0, 1), pl.ds(1, heads - 1)
    firsts = [
        pltpu.make_async_copy(
            weight_2.at[side, part], held.at[side, part], ready.at[side, place]
        )
        for place, part in enumerate((lead, rest))
    ]
    for copy in firsts:
        copy.start()

    @pl.when(crossed)
    def _():
        copies(2).start()

    def summed(head):
        if head < 2:
            firsts[head].wait()
        return near_ref[head] + weighed(
            held, mark_2, level_ref, v2_ref[side * heads + head], side, head, heads, side
        )

    def write(head, block):
        turned = jnp.transpose(block, (1, 0)).astype(jnp.bfloat16)
        out_ref[head * 2] = turned[:rows]
        out_ref[head * 2 + 1] = turned[rows:]

    @pl.when(crossed)
    def _():
        for head in range(heads):
            sum_ref[head] = summed(head)
        copies(2).wait()
        for head in range(heads):
            write(
                head,
                sum_ref[head]
                + weighed(
                    held, mark_2, level_ref, v2_ref[(1 - side) * heads + head],
                    side, head, heads, 2,
                ),
            )

    @pl.when(jnp.logical_not(crossed))
    def _():
        for head in range(heads):
            write(head, summed(head))


def call(kernel, out_shape, scalars, count, flops, scratch=(), far_in=(), far_out=()):
    def run(*operands):
        return pl.pallas_call(
            kernel,
            out_shape=out_shape,
            in_specs=[SMEM] * scalars
            + [HBM if i in far_in else VMEM for i in range(scalars, count)],
            out_specs=tuple(
                HBM if i in far_out else VMEM for i in range(len(out_shape))
            ),
            scratch_shapes=list(scratch),
            cost_estimate=pl.CostEstimate(flops=flops, bytes_accessed=0, transcendentals=0),
            compiler_params=pltpu.CompilerParams(vmem_limit_bytes=VMEM_LIMIT),
        )(*operands)

    return run


def by_head(tensor):
    return lax.optimization_barrier(jnp.transpose(tensor, (1, 0, 2)))


def half_of(tensor, core):
    part = tensor.shape[0] // CORES
    return jnp.where(core == 0, tensor[:part], tensor[part:])


def device_part(queries, keys, values, doc_lengths):
    rows, query_heads, width = queries.shape[1:]
    key_heads = keys.shape[2]
    heads = key_heads // CORES
    members = query_heads // key_heads
    devices = lax.axis_size(DP_SEQ)
    core = lax.axis_index("seq_2")
    chip = lax.axis_index(CHIP)
    f32, bf16 = jnp.float32, jnp.bfloat16
    shape = jax.ShapeDtypeStruct
    spot = jnp.stack([chip, core]).astype(jnp.int32)

    k_all = by_head(keys[0])
    k1_own = up_chip(half_of(k_all, core))
    k0_other = swapped(half_of(k_all, 1 - core))
    k1_other = up_chip(k0_other)
    k2_own = up_chip(k1_own)
    q_all = by_head(queries[0])
    v_all = by_head(values[0])
    give = jnp.concatenate([half_of(q_all, 1 - core), half_of(v_all, 1 - core)], axis=0)
    got = swapped(give)

    table = shape((3 * CORES, rows, width), f32)
    lane = jnp.arange(width // 2, dtype=f32)
    frequency = rope_base ** (-2.0 * lane / width)
    frequency = jnp.concatenate([frequency, frequency])[None, :]
    cos_table, sin_table = call(table_kernel, (table, table), 2, 3, TABLE_FLOPS)(
        doc_lengths, spot, frequency
    )
    k2_other = up_chip(k1_other)

    stats = shape((CORES * heads, members * rows), f32)
    q_shape = shape((CORES, heads, members * rows, width), bf16)
    key_scratch = pltpu.VMEM((CORES, heads, rows, width), bf16)

    def slots(count):
        return (
            pltpu.HBM((count, heads, rows, members * rows), bf16),
            shape((count, heads, members * rows), f32),
        )

    def staged(count):
        return (
            key_scratch,
            pltpu.VMEM((count, heads, rows, members * rows), bf16),
            pltpu.SemaphoreType.DMA((count, heads)),
        )

    v_shape = shape((CORES * heads, rows, width), bf16)
    query_rot, v0, weight_0, mark_0, peak, total = call(
        first_kernel, (q_shape, v_shape, *slots(3), stats, stats), 2, 9, FIRST_FLOPS,
        staged(3), far_out=(2,),
    )(doc_lengths, spot, cos_table, sin_table, k_all, k0_other, q_all, v_all, got)
    v1 = up_chip(v0)
    v2 = up_chip(v1)
    weight_1, mark_1, peak, total = call(
        next_kernel, (*slots(4), stats, stats), 2, 9, NEXT_FLOPS, staged(4),
        far_out=(0,),
    )(doc_lengths, spot, cos_table, sin_table, k1_own, k1_other, query_rot, peak, total)
    weight_2, mark_2, level, squares = call(
        last_kernel,
        (*slots(3), stats, shape((lax.axis_size(("seq_1", "seq_2")), width), f32)),
        2,
        9,
        NEXT_FLOPS,
        (pltpu.VMEM(stats.shape, f32), pltpu.VMEM(stats.shape, f32), *staged(3)),
        far_out=(0,),
    )(doc_lengths, spot, cos_table, sin_table, k2_own, k2_other, query_rot, peak, total)
    squares = lax.all_to_all(squares, ("seq_1", "seq_2"), 0, 0)
    across = ("dp_0", "dp_1", "seq_0")
    squares = jnp.sum(squares, axis=0, keepdims=True)
    squares = jnp.broadcast_to(squares, (lax.axis_size(across), width))
    squares = lax.all_to_all(squares, across, 0, 0)
    squares = jnp.sum(squares, axis=0, keepdims=True)
    z_loss = squares[0, 0] / (devices * rows * query_heads)

    weight_0, weight_1, weight_2 = (
        pltpu.with_memory_space_constraint(array, pltpu.HBM)
        for array in (weight_0, weight_1, weight_2)
    )
    sum_shape = shape((heads, width, members * rows), f32)
    near = call(
        near_kernel, (sum_shape, sum_shape), 1, 8, NEAR_FLOPS,
        (*staged(3)[1:2], *staged(4)[1:2], *staged(3)[2:], *staged(4)[2:]),
        far_in=(2, 4),
    )(spot, level, weight_0, mark_0, weight_1, mark_1, v0, v1)
    out_shape = shape((heads * members, rows, width), bf16)
    own, other = (
        call(
            functools.partial(far_kernel, side), (out_shape,), 1, 6, NEAR_FLOPS,
            (pltpu.VMEM(sum_shape.shape, f32), *staged(3)[1:]),
            far_in=(2,),
        )(spot, level, weight_2, mark_2, v2, near[side])[0]
        for side in range(2)
    )
    partner = swapped(other)
    low = jnp.where(core == 0, own, partner)
    high = jnp.where(core == 0, partner, own)
    attended = jnp.transpose(jnp.concatenate([low, high], axis=0), (1, 0, 2))
    return (attended[None], z_loss)


VMEM_LIMIT = 20 * 1024 * 1024
TABLE_FLOPS = 4_000_000
FIRST_FLOPS = 6_000_000
NEXT_FLOPS = 6_000_000
NEAR_FLOPS = 3_000_000


def solution(mesh):
    torus = Mesh(mesh.devices.reshape(8, 2, 2, 8, 2), ("dp_0", "dp_1", "seq_0", "seq_1", "seq_2"))
    in_specs = (P(DP, SEQ, None, None), P(DP, SEQ, None, None), P(DP, SEQ, None, None), P(DP, None))
    out_specs = (P(DP, SEQ, None, None), P())
    return jax.shard_map(
        device_part, mesh=torus, in_specs=in_specs, out_specs=out_specs, check_vma=False
    )
```
